128 devices in a mesh: rows: 16 (over z_hi, x, core), cols: 8 (over y, z_lo).
Axes of the slice: x: 4, y: 4, z: 4 (z_hi: 2, z_lo: 2; z = z_hi * 2 + z_lo), core: 2. Of those that a mesh axis runs over, the one named last changes fastest.
Arguments:
- block_values: bfloat16 [65536, 128], P(('rows', 'cols')), may hold values from -6 to 6
- block_length: int32 [65536], P(('rows', 'cols')), may hold values from 1 to 128
- block_owner: int32 [65536], P(('rows', 'cols')), may hold values from 0 to 16383, as said below
- block_second: int32 [65536], P(('rows', 'cols')), may hold values from 0 to 16383, as said below
- block_third: int32 [65536, 128], P(('rows', 'cols')), may hold values from 0 to 32767
- live_blocks: int32 [128], P(('rows', 'cols')), may hold values from 1 to 512, as said below
- second_factor: bfloat16 [16384, 256], P('cols', 'rows')
- third_factor: bfloat16 [32768, 256], P('cols', 'rows'), may hold values from -6 to 6
Outputs:
- first_factor: float32 [16384, 256], P('cols', 'rows')
The draws below stay inside these ranges and needn't reach their ends.
Inputs may be any that keep to these rules, and one draw needn't show every extreme that they name: `block_owner`: slot b lies on device d = b // 512 with index r along rows; its row lies in r * 16384 // 16 up to (r + 1) * 16384 // 16 - 1, the device's mode-1 slab. `block_second`: slot b lies on device d = b // 512 with index c along cols; its row lies in c * 16384 // 8 up to (c + 1) * 16384 // 8 - 1. `live_blocks`: some device uses all 512 slots in every draw.
All inputs are finite; a program needn't handle non-finite values.
Results may differ from the reference program's by a relative error of at most 0.0003.
Values may be sent and summed in bfloat16 or wider, within the bound.
A program may use at most 128 MiB of HBM per device.

```python
import jax
import jax.numpy as jnp
from jax import lax

R = 256
L = 128
NB_DEV = 512
BLOCKS = 65536
I = 16384
J = 16384
K = 32768
N_ROWS = 16
N_COLS = 8
DEVICES = 128


def draw_block_owner(key, part):
    slot = jnp.arange(NB_DEV * DEVICES, dtype=jnp.int32)
    device = slot // NB_DEV
    slab = I // N_ROWS
    offset = jax.random.randint(key, (NB_DEV * DEVICES,), 0, slab, dtype=jnp.int32)
    return device // N_COLS * slab + offset


def draw_block_second(key, part):
    slot = jnp.arange(NB_DEV * DEVICES, dtype=jnp.int32)
    device = slot // NB_DEV
    span = J // N_COLS
    offset = jax.random.randint(jax.random.fold_in(key, 7), (NB_DEV * DEVICES,), 0, span, dtype=jnp.int32)
    return device % N_COLS * span + offset


def draw_live_blocks(key, part):
    first, second = jax.random.split(jax.random.fold_in(key, 11))
    counts = jax.random.randint(first, (DEVICES,), 1, NB_DEV + 1, dtype=jnp.int32)
    full = jax.random.randint(second, (), 0, DEVICES, dtype=jnp.int32)
    return jnp.where(jnp.arange(DEVICES, dtype=jnp.int32) == full, NB_DEV, counts)


def draw_second_factor(key, part):
    first = jax.random.fold_in(jax.random.fold_in(key, 13), 0)
    third = jax.random.fold_in(jax.random.fold_in(key, 13), 2)
    trend = 3.0 ** (jnp.arange(J, dtype=jnp.float32) / J)
    scale = trend * 10.0 ** jax.random.uniform(first, (J,), jnp.float32)
    base = jax.random.normal(third, (J, R), jnp.float32)
    return (scale[:, None] * base).astype(jnp.bfloat16)


def place_ends(drawn, stream_key, low, top_value):
    longest = drawn.shape.index(max(drawn.shape))
    spots = []
    for shift in (0, 1):
        where = [jax.random.randint(jax.random.fold_in(stream_key, axis), (), 0, length) for axis, length in enumerate(drawn.shape)]
        where[longest] = (where[longest] + shift) % drawn.shape[longest]
        spots.append(tuple(where))
    return drawn.at[spots[0]].set(low).at[spots[1]].set(top_value)


def steps_of(key, dims, cuts, smallest, high):
    gain = 1.0
    for dim, blocks in cuts:
        draws = jax.random.uniform(jax.random.fold_in(jax.random.fold_in(key, 6), dim), (blocks,), jnp.float32, smallest / len(cuts), high / len(cuts))
        gain = gain * jnp.repeat(jnp.exp(draws), dims[dim] // blocks).reshape((-1,) + (1,) * (len(dims) - 1 - dim))
    return gain


def scatter_about(own_key, dims, deviation, reach, shards=(), kind=jnp.bfloat16):
    values = jax.random.normal(own_key, dims, jnp.float32) * deviation
    if len(shards) > 0:
        values = steps_of(own_key, dims, shards, -0.22, 0.18) * values
    return jnp.clip(values, min=-reach, max=reach).astype(kind)


def setup_inputs(seed: int = 0) -> dict:
    key_of = jax.random.split(jax.random.key(seed), 9)
    return {
        "block_values": scatter_about(key_of[0], (BLOCKS, L), 1.0, 6.0, ((0, 128),)),
        "block_length": place_ends(jax.random.randint(key_of[1], (BLOCKS,), 1, L + 1), jax.random.fold_in(key_of[1], 1), 1, L).astype(jnp.int32),
        "block_owner": draw_block_owner(jax.random.fold_in(key_of[8], 71), 0),
        "block_second": draw_block_second(jax.random.fold_in(key_of[8], 71), 0),
        "block_third": place_ends(jax.random.randint(key_of[4], (BLOCKS, L), 0, K), jax.random.fold_in(key_of[4], 1), 0, K - 1).astype(jnp.int32),
        "live_blocks": draw_live_blocks(jax.random.fold_in(key_of[8], 71), 0),
        "second_factor": draw_second_factor(jax.random.fold_in(key_of[8], 71), 0),
        "third_factor": scatter_about(key_of[7], (K, R), 1.0, 6.0, ((0, 8), (1, 16))),
    }


def reference(block_values, block_length, block_owner, block_second, block_third, live_blocks, second_factor, third_factor):
    nblk = block_values.shape[0]
    width = block_values.shape[1]
    group = min(nblk, 512)
    position = jnp.arange(nblk, dtype=jnp.int32)
    live_block = position % NB_DEV < live_blocks[position // NB_DEV]
    lane = jnp.arange(width, dtype=jnp.int32)
    live = (lane[None, :] < block_length[:, None]) & live_block[:, None]
    masked = jnp.where(live, block_values, jnp.zeros((), jnp.bfloat16))
    steps = nblk // group

    def accumulate(total, pieces):
        values, third, second, owner = pieces
        rows = third_factor[third].astype(jnp.float32)
        fold = jnp.einsum('gt,gtr->gr', values.astype(jnp.float32), rows)
        contrib = second_factor[second].astype(jnp.float32) * fold
        return (total.at[owner].add(contrib), None)
    pieces = (masked.reshape(steps, group, width), block_third.reshape(steps, group, width), block_second.reshape(steps, group), block_owner.reshape(steps, group))
    start = jnp.zeros((I, R), jnp.float32)
    mttkrp, unused = lax.scan(accumulate, start, pieces)
    contract = (((0,), (0,)), ((), ()))
    gram_second = lax.dot_general(second_factor.astype(jnp.float32), second_factor.astype(jnp.float32), contract, preferred_element_type=jnp.float32) / J
    gram_third = lax.dot_general(third_factor.astype(jnp.float32), third_factor.astype(jnp.float32), contract, preferred_element_type=jnp.float32) / K
    gram = gram_second * gram_third
    factor = jnp.linalg.cholesky(gram)
    return jax.scipy.linalg.cho_solve((factor, True), mttkrp.T).T
```

```python
import jax
import jax.numpy as jnp
from jax import lax
from jax.experimental import pallas as pl
from jax.experimental.pallas import tpu as pltpu
from jax.sharding import PartitionSpec as P

F32 = jnp.float32
BF = jnp.bfloat16
MESH = pl.DeviceIdType.MESH
NT = (((1,), (1,)), ((), ()))
NN = (((1,), (0,)), ((), ()))
HIGH = lax.Precision.HIGHEST
VMEM = pltpu.VMEM
ANY = pl.BlockSpec(memory_space=pl.ANY)
INV = pl.BlockSpec(memory_space=pltpu.VMEM)

PARTS = ((0, 1408), (1408, 1408), (2816, 1280))
ORDERS = ("xyz", "yzx", "zxy")
SEMS = 28 * 3 + 16 * 3


def place():
    r, c = lax.axis_index("rows"), lax.axis_index("cols")
    return {"z": lax.div(r, 8) * 2 + lax.rem(c, 2), "x": lax.rem(lax.div(r, 2), 4), "k": lax.rem(r, 2), "y": lax.div(c, 2)}


def device(at):
    return (lax.div(at["z"], 2) * 8 + at["x"] * 2 + at["k"], at["y"] * 2 + lax.rem(at["z"], 2))


def moved(at, dim, step):
    return {**at, dim: lax.rem(at[dim] + step, 4)}


class Gather:
    def __init__(self, t, send, recv):
        self.t, self.send, self.recv = t, send, recv
        self.me = place()
        self.used = 0
        self.sent = []

    def block(self, part, at, half=None):
        start, size = PARTS[part]
        if half is not None:
            first = (size // 128 // 2) * 128
            start, size = (start, first) if half == 0 else (start + first, size - first)
        return self.t.at[at["z"], at["x"], at["k"], at["y"], :, pl.ds(start, size)]

    def set_of(self, part, at, whole):
        start, size = PARTS[part]
        return self.t.at[*[slice(None) if d in whole else at[d] for d in "zxky"], :, pl.ds(start, size)]

    def new(self):
        self.used += 1
        return self.used - 1

    def copy(self, ref, n, to):
        c = pltpu.make_async_remote_copy(ref, ref, self.send.at[n], self.recv.at[n], device_id=device(to), device_id_type=MESH)
        c.start()
        self.sent.append(c)

    def arrived(self, ref, n):
        pltpu.make_async_remote_copy(ref, ref, self.send.at[n], self.recv.at[n], device_id=device(self.me), device_id_type=MESH).wait_recv()

    def run(self):
        me = self.me
        FORE, BACK = 1, 3
        parts = range(3)
        one = {(p, s): self.new() for p in parts for s in (FORE, BACK)}
        onef = {(p, s): self.new() for p in parts for s in (FORE, BACK)}
        two = {(p, o, s): self.new() for p in parts for o in range(4) for s in (FORE, BACK)}
        twof = {(p, o): self.new() for p in parts for o in range(4)}
        three = {(p, o, s): self.new() for p in parts for o in range(4) for s in (FORE, BACK)}
        threef = {(p, o): self.new() for p in parts for o in range(4)}
        core = {(p, a, b): self.new() for p in parts for a in range(4) for b in range(4)}
        other = {**me, "k": 1 - me["k"]}

        def dims(p):
            return ORDERS[p]

        def at1(p, a):
            return moved(me, dims(p)[0], a)

        def at2(p, a, b):
            return moved(at1(p, a), dims(p)[1], b)

        def set3(p, b, c, k=None):
            d = dims(p)
            at = moved(moved(me, d[1], b), d[2], c)
            if k is not None:
                at = {**at, "k": k}
            return self.set_of(p, at, d[0])

        def to(p, i, s):
            return moved(me, dims(p)[i], s)

        def cross(p, b, c):
            self.copy(set3(p, b, c), core[p, b, c], other)

        for p in parts:
            for s in (FORE, BACK):
                self.copy(self.block(p, me), one[p, s], to(p, 0, s))
        for p in parts:
            for s in (FORE, BACK):
                self.copy(self.block(p, me), two[p, 0, s], to(p, 1, s))
        for p in parts:
            for s in (FORE, BACK):
                back = 4 - s
                self.arrived(self.block(p, at1(p, back)), one[p, s])
                self.copy(self.block(p, at1(p, back), half=0 if s == FORE else 1), onef[p, s], to(p, 0, s))
                for s2 in (FORE, BACK):
                    self.copy(self.block(p, at1(p, back)), two[p, back, s2], to(p, 1, s2))
        for p in parts:
            for s in (FORE, BACK):
                self.arrived(self.block(p, at1(p, 2), half=0 if s == FORE else 1), onef[p, s])
            for s2 in (FORE, BACK):
                self.copy(self.block(p, at1(p, 2)), two[p, 2, s2], to(p, 1, s2))
            for s3 in (FORE, BACK):
                self.copy(set3(p, 0, 0), three[p, 0, s3], to(p, 2, s3))
            cross(p, 0, 0)
        FIRST = {FORE: (0, 3), BACK: (1, 2)}
        for p in parts:
            for o in (0, 3, 1, 2):
                for s in (FORE, BACK):
                    back = 4 - s
                    self.arrived(self.block(p, at2(p, o, back)), two[p, o, s])
                    if o in FIRST[s]:
                        self.copy(self.block(p, at2(p, o, back)), twof[p, o], to(p, 1, s))
        for p in parts:
            for b in (3, 1):
                for s3 in (FORE, BACK):
                    self.copy(set3(p, b, 0), three[p, b, s3], to(p, 2, s3))
                cross(p, b, 0)
        for p in parts:
            for o in (0, 3, 1, 2):
                self.arrived(self.block(p, at2(p, o, 2)), twof[p, o])
            for s3 in (FORE, BACK):
                self.copy(set3(p, 2, 0), three[p, 2, s3], to(p, 2, s3))
            cross(p, 2, 0)
        yield
        for b in (0, 3, 1, 2):
            for p in parts:
                for s in (FORE, BACK):
                    back = 4 - s
                    self.arrived(set3(p, b, back), three[p, b, s])
                    if b in FIRST[s]:
                        self.copy(set3(p, b, back), threef[p, b], to(p, 2, s))
                    cross(p, b, back)
        yield
        for b in (0, 3, 1, 2):
            for p in parts:
                self.arrived(set3(p, b, 2), threef[p, b])
                cross(p, b, 2)
        for p in parts:
            for a in range(4):
                for b in range(4):
                    self.arrived(set3(p, a, b, k=1 - me["k"]), core[p, a, b])
        for c in self.sent:
            c.wait_send()


def send_to(src, dst, ssem, rsem, to):
    c = pltpu.make_async_remote_copy(src, dst, ssem, rsem, device_id=to, device_id_type=MESH)
    c.start()
    return c


def k1_body(piece, spiece, t, s_out, gs_out, s_vm, part, parts, mine, send, recv, ssem, srecv, csem, crecv, gsem, grecv, lsem):
    g = Gather(t, send, recv)
    me = g.me
    r, c = lax.axis_index("rows"), lax.axis_index("cols")
    cp = pltpu.make_async_copy(piece, t.at[me["z"], me["x"], me["k"], me["y"]], lsem.at[0])
    cp.start()
    cs = pltpu.make_async_copy(spiece, s_vm.at[r], lsem.at[1])
    cs.start()
    sent = []
    for i in range(1, 16):
        to = lax.rem(r + i, 16)
        sent.append(send_to(spiece, s_vm.at[r], ssem.at[i - 1], srecv.at[i - 1], (to, c)))
    cp.wait()
    cs.wait()
    run = g.run()
    next(run)
    for i in range(1, 16):
        got = s_vm.at[lax.rem(r + 16 - i, 16)]
        pltpu.make_async_remote_copy(got, got, ssem.at[i - 1], srecv.at[i - 1], device_id=(r, c), device_id_type=MESH).wait_recv()
    whole = s_vm[...].reshape(256, 2048)
    chunk = lax.dot_general(s_vm[r], whole, NT, preferred_element_type=F32)
    part[...] = chunk
    parts[c] = chunk
    for i in range(1, 8):
        sent.append(send_to(part, parts.at[c], csem.at[i - 1], crecv.at[i - 1], (r, lax.rem(c + i, 8))))
    out = pltpu.make_async_copy(s_vm, s_out, lsem.at[2])
    out.start()
    next(run)
    for i in range(1, 8):
        got = parts.at[lax.rem(c + 8 - i, 8)]
        pltpu.make_async_remote_copy(got, got, csem.at[i - 1], crecv.at[i - 1], device_id=(r, c), device_id_type=MESH).wait_recv()
    mine[...] = sum(parts[i] for i in range(8))
    keep = pltpu.make_async_copy(mine, gs_out.at[r], lsem.at[3])
    keep.start()
    for i in range(1, 16):
        sent.append(send_to(mine, gs_out.at[r], gsem.at[i - 1], grecv.at[i - 1], (lax.rem(r + i, 16), c)))
    for _ in run:
        pass
    for i in range(1, 16):
        got = gs_out.at[lax.rem(r + 16 - i, 16)]
        pltpu.make_async_remote_copy(got, got, gsem.at[i - 1], grecv.at[i - 1], device_id=(r, c), device_id_type=MESH).wait_recv()
    out.wait()
    keep.wait()
    for x in sent:
        x.wait_send()


def k1(piece, spiece):
    D = pltpu.SemaphoreType.DMA
    return pl.pallas_call(
        k1_body,
        out_shape=(
            jax.ShapeDtypeStruct((4, 4, 2, 4, 16, 4096), BF),
            jax.ShapeDtypeStruct((16, 16, 2048), BF),
            jax.ShapeDtypeStruct((16, 16, 256), F32),
        ),
        in_specs=[ANY, ANY],
        out_specs=(ANY, ANY, ANY),
        scratch_shapes=[
            VMEM((16, 16, 2048), BF), VMEM((16, 256), F32), VMEM((8, 16, 256), F32), VMEM((16, 256), F32),
            D((SEMS,)), D((SEMS,)), D((15,)), D((15,)), D((7,)), D((7,)), D((15,)), D((15,)), D((4,)),
        ],
        compiler_params=pltpu.CompilerParams(has_side_effects=True),
        name="gather_factors",
    )(piece, spiece)

UB = 16
PAD = 136


def spread_step(step, base, q_ref, p_ref, v_ref, wf, whi, wlo):
    iq = lax.broadcasted_iota(jnp.int32, (128, 128), 0).astype(F32).astype(BF)
    ip = lax.broadcasted_iota(jnp.int32, (256, 128), 0).astype(F32).astype(BF)
    zero = jnp.zeros((128, 128), BF)
    one = jnp.ones((), BF)

    def row(ref, b, n):
        r = jnp.broadcast_to(ref[pl.ds(b, 1), :], (16, 128)).astype(BF)
        return jnp.concatenate([r] * (n // 16), axis=0)

    for pair in range(UB // 2):
        qs, ps = [], []
        for j in range(2):
            b = base + step * UB + 2 * pair + j
            qm = iq == row(q_ref, b, 128)
            qs.append(jnp.where(qm, row(v_ref, b, 128), zero))
            ps.append(jnp.where(ip == row(p_ref, b, 256), one, jnp.zeros((), BF)))
        lhs = jnp.concatenate([jnp.concatenate([qs[0], zero], 1), jnp.concatenate([zero, qs[1]], 1)], 0)
        rhs = jnp.concatenate(ps, 1)
        w = lax.dot_general(lhs, rhs, NT, preferred_element_type=F32)
        for j in range(2):
            for h in range(2):
                wf[h, pl.ds((2 * pair + j) * PAD, 128), :] = w[j * 128:(j + 1) * 128, h * 128:(h + 1) * 128]

    rows = pl.ds(pl.multiple_of(step * UB, UB), UB)

    def split(q8, _):
        for i in range(8):
            q = q8 * 8 + i
            for h in range(2):
                f = wf[h, pl.ds(q, UB, stride=PAD), :]
                hi = f.astype(BF)
                lo = (f - hi.astype(F32)).astype(BF)
                lanes = pl.ds(pl.multiple_of(q * 256, 256) + h * 128, 128)
                whi[rows, lanes] = hi
                wlo[rows, lanes] = lo
        return 0

    lax.fori_loop(0, 16, split, 0)


GRP = 256
KC = 2048


def k2_body(q_ref, p_ref, v_ref, sec_ref, own_ref, t_hbm, s_ref, out_ref, gt_ref, wf, whi, wlo, tbuf, fold, tsem):
    cps = []
    for c in range(8):
        for z in range(2):
            cps.append(pltpu.make_async_copy(t_hbm.at[z * 2 + c % 2, :, :, c // 2], tbuf.at[c, z], tsem.at[c * 2 + z]))
            cps[-1].start()
    gt_ref[...] = jnp.zeros((256, 256), F32)
    for g in range(512 // GRP):
        def st(i, _):
            spread_step(i, g * GRP, q_ref, p_ref, v_ref, wf, whi, wlo)
            return 0
        lax.fori_loop(0, GRP // UB, st, 0)
        if g == 0:
            for c in cps:
                c.wait()
        grow = pl.ds(g * GRP, GRP)
        fold[grow, :] = jnp.zeros((GRP, 256), F32)

        def mm(i, _):
            c = lax.div(i, 4096 // KC)
            k0 = pl.multiple_of(lax.rem(i, 4096 // KC) * KC, KC)
            t = tbuf[c, :, :, :, :, pl.ds(k0, KC)].reshape(256, KC)
            ks = pl.ds(pl.multiple_of(i * KC, KC), KC)
            lhs = jnp.concatenate([whi[:, ks], wlo[:, ks]] + ([t] if g == 0 else []), 0)
            r = lax.dot_general(lhs, t, NT, preferred_element_type=F32)
            fold[grow, :] += r[:GRP] + r[GRP:2 * GRP]
            if g == 0:
                gt_ref[...] += r[2 * GRP:]
            return 0
        lax.fori_loop(0, 32768 // KC, mm, 0)
    one, zero = jnp.ones((), BF), jnp.zeros((), BF)
    ij = lax.broadcasted_iota(jnp.int32, (2048, 512), 0)
    pick = jnp.where(ij == sec_ref[...], one, zero)
    second = lax.dot_general(s_ref[...].reshape(256, 2048), pick, NN, preferred_element_type=F32)
    contrib = second * fold[...].T
    hi = contrib.astype(BF)
    rest = contrib - hi.astype(F32)
    mid = rest.astype(BF)
    low = (rest - mid.astype(F32)).astype(BF)
    ii = lax.broadcasted_iota(jnp.int32, (1024, 512), 0)
    put = jnp.where(ii == own_ref[...], one, zero)
    r = lax.dot_general(jnp.concatenate([hi, mid, low], 0), put, NT, preferred_element_type=F32)
    total = r[:256] + (r[256:512] + r[512:])
    for c in range(8):
        out_ref[c] = total[:, c * 128:(c + 1) * 128]


def k2(q, p, v, sec, own, t, s):
    return pl.pallas_call(
        k2_body,
        out_shape=(jax.ShapeDtypeStruct((8, 256, 128), F32), jax.ShapeDtypeStruct((256, 256), F32)),
        in_specs=[INV] * 5 + [ANY, INV],
        out_specs=(INV, INV),
        scratch_shapes=[
            VMEM((2, UB * PAD, 128), F32),
            VMEM((GRP, 32768), BF),
            VMEM((GRP, 32768), BF),
            VMEM((8, 2, 4, 2, 16, 4096), BF),
            VMEM((512, 256), F32),
            pltpu.SemaphoreType.DMA((16,)),
        ],
        compiler_params=pltpu.CompilerParams(vmem_limit_bytes=67043328),
        name="spread_fold",
    )(q, p, v, sec, own, t, s)


def inverse_body(gs_ref, gt_ref, out_ref, a_ref, x_ref):
    gram = (gs_ref[...].reshape(256, 256) / 16384) * (gt_ref[...] / 32768)
    eye = (lax.broadcasted_iota(jnp.int32, (256, 256), 0) == lax.broadcasted_iota(jnp.int32, (256, 256), 1)).astype(F32)
    diag = gram * eye
    down = 1 / jnp.sqrt(jnp.sum(diag, axis=1, keepdims=True))
    along = 1 / jnp.sqrt(jnp.sum(diag, axis=0, keepdims=True))
    a = gram * down * along
    a_ref[...] = a
    bound = jnp.max(jnp.sum(jnp.abs(a), axis=0))
    x_ref[...] = eye * (2 / (1 + bound))

    def dot(u, w):
        return lax.dot_general(u, w, NN, precision=HIGH, preferred_element_type=F32)

    def go(state):
        return (state[0] < 64) & (state[1] > 1e-4)

    def step(state):
        x = x_ref[...]
        rest = eye - dot(a_ref[...], x)
        x_ref[...] = x + dot(x, rest)
        return state[0] + 1, jnp.max(jnp.abs(rest))

    lax.while_loop(go, step, (0, jnp.float32(1.0)))
    out_ref[...] = x_ref[...] * down * along


def inverse(gs, gt):
    return pl.pallas_call(
        inverse_body,
        out_shape=jax.ShapeDtypeStruct((256, 256), F32),
        in_specs=[INV, INV],
        out_specs=INV,
        scratch_shapes=[VMEM((256, 256), F32), VMEM((256, 256), F32)],
        name="gram_inverse",
    )(gs, gt)


def k3_body(part, inv, out, got, x, rsem, rrecv, xsem, xrecv, lsem):
    r, c = lax.axis_index("rows"), lax.axis_index("cols")
    sent = []
    for i in range(1, 8):
        to = lax.rem(c + i, 8)
        sent.append(send_to(part.at[to], got.at[i - 1], rsem.at[i - 1], rrecv.at[i - 1], (r, to)))
    total = part[c]
    for i in range(7):
        pltpu.make_async_remote_copy(got.at[i], got.at[i], rsem.at[i], rrecv.at[i], device_id=(r, c), device_id_type=MESH).wait_recv()
        total = total + got[i]
    solved = lax.dot_general(inv[...], total, NN, precision=HIGH, preferred_element_type=F32)
    x[...] = solved.reshape(16, 16, 128)
    home = lax.div(r, 2)
    slot = lax.rem(r, 2) * 8 + c
    mine = home == c
    lanes = pl.ds(pl.multiple_of(slot * 128, 128), 128)
    for i in range(1, 16):
        to = lax.rem(r + i, 16)
        sent.append(send_to(x.at[to], out.at[:, lanes], xsem.at[i], xrecv.at[slot], (to, home)))

    near = pltpu.make_async_copy(x.at[r], out.at[:, lanes], lsem)
    far = pltpu.make_async_remote_copy(x.at[r], out.at[:, lanes], xsem.at[0], xrecv.at[slot], device_id=(r, home), device_id_type=MESH)

    @pl.when(mine)
    def _():
        near.start()

    @pl.when(jnp.logical_not(mine))
    def _():
        far.start()

    for i in range(16):
        there = out.at[:, pl.ds(i * 128, 128)]
        take = pltpu.make_async_remote_copy(there, there, xsem.at[0], xrecv.at[i], device_id=(r, c), device_id_type=MESH)

        @pl.when(jnp.logical_not(mine & (slot == i)))
        def _():
            take.wait_recv()

    @pl.when(mine)
    def _():
        near.wait()

    @pl.when(jnp.logical_not(mine))
    def _():
        far.wait_send()

    for s in sent:
        s.wait_send()


def k3(part, inv):
    D = pltpu.SemaphoreType.DMA
    return pl.pallas_call(
        k3_body,
        out_shape=jax.ShapeDtypeStruct((16, 2048), F32),
        in_specs=[INV, INV],
        out_specs=INV,
        scratch_shapes=[VMEM((7, 256, 128), F32), VMEM((16, 16, 128), F32), D((7,)), D((7,)), D((16,)), D((16,)), D(())],
        compiler_params=pltpu.CompilerParams(has_side_effects=True),
        name="reduce_solve_place",
    )(part, inv)


def per_device(values, length, owner, second, third, live_blocks, second_factor, third_factor):
    r, c = lax.axis_index("rows"), lax.axis_index("cols")
    lane = jnp.arange(128, dtype=jnp.int32)
    slot = jnp.arange(512, dtype=jnp.int32)
    live = (lane[None, :] < length[:, None]) & (slot < live_blocks[0])[:, None]
    v = jnp.where(live, values, jnp.zeros((), BF)).astype(F32)
    q = (third >> 8).astype(F32)
    p = (third & 255).astype(F32)
    sec = (second - c * 2048).reshape(1, 512)
    own = (owner - r * 1024).reshape(1, 512)
    t, s, gs = k1(third_factor.T, second_factor.T)
    part, gt = k2(q, p, v, sec, own, t, s)
    inv = inverse(gs, gt)
    return k3(part, inv).T


def solution(mesh):
    both = P(("rows", "cols"))
    wide = P(("rows", "cols"), None)
    return jax.shard_map(
        per_device,
        mesh=mesh,
        in_specs=(wide, both, both, both, wide, both, P("cols", "rows"), P("cols", "rows")),
        out_specs=P("cols", "rows"),
        check_vma=False,
    )
```

```python
import jax
import jax.numpy as jnp
from jax import lax
from jax.experimental import pallas as pl
from jax.experimental.pallas import tpu as pltpu
from jax.sharding import PartitionSpec as P

F32 = jnp.float32
BF = jnp.bfloat16
MESH = pl.DeviceIdType.MESH
NT = (((1,), (1,)), ((), ()))
NN = (((1,), (0,)), ((), ()))
HIGH = lax.Precision.HIGHEST
VMEM = pltpu.VMEM
ANY = pl.BlockSpec(memory_space=pl.ANY)
INV = pl.BlockSpec(memory_space=pltpu.VMEM)

PARTS = ((0, 1408), (1408, 1408), (2816, 1280))
ORDERS = ("xyz", "yzx", "zxy")
SEMS = 28 * 3 + 16 * 3


def place():
    r, c = lax.axis_index("rows"), lax.axis_index("cols")
    return {"z": lax.div(r, 8) * 2 + lax.rem(c, 2), "x": lax.rem(lax.div(r, 2), 4), "k": lax.rem(r, 2), "y": lax.div(c, 2)}


def device(at):
    return (lax.div(at["z"], 2) * 8 + at["x"] * 2 + at["k"], at["y"] * 2 + lax.rem(at["z"], 2))


class Gather:
    def __init__(self, t, send, recv):
        self.t, self.send, self.recv = t, send, recv
        self.me = me = place()
        self.mine = device(me)
        self.steps = {d: [me[d], *(lax.rem(me[d] + i, 4) for i in (1, 2, 3))] for d in "zxy"}
        self.other = {**me, "k": 1 - me["k"]}
        self.used = 0
        self.sent = []

    def moved(self, at, dim, step):
        return {**at, dim: self.steps[dim][step]}

    def block(self, part, at, half=None):
        start, size = PARTS[part]
        if half is not None:
            first = (size // 128 // 2) * 128
            start, size = (start, first) if half == 0 else (start + first, size - first)
        return self.t.at[at["z"], at["x"], at["k"], at["y"], :, pl.ds(start, size)]

    def set_of(self, part, at, whole):
        start, size = PARTS[part]
        return self.t.at[*[slice(None) if d in whole else at[d] for d in "zxky"], :, pl.ds(start, size)]

    def new(self):
        self.used += 1
        return self.used - 1

    def copy(self, ref, n, to):
        c = pltpu.make_async_remote_copy(ref, ref, self.send.at[n], self.recv.at[n], device_id=device(to), device_id_type=MESH)
        c.start()
        self.sent.append((ref, n))

    def arrived(self, ref, n):
        pltpu.make_async_remote_copy(ref, ref, self.send.at[n], self.recv.at[n], device_id=self.mine, device_id_type=MESH).wait_recv()

    def run(self):
        me = self.me
        FORE, BACK = 1, 3
        parts = range(3)
        one = {(p, s): self.new() for p in parts for s in (FORE, BACK)}
        onef = {(p, s): self.new() for p in parts for s in (FORE, BACK)}
        two = {(p, o, s): self.new() for p in parts for o in range(4) for s in (FORE, BACK)}
        twof = {(p, o): self.new() for p in parts for o in range(4)}
        three = {(p, o, s): self.new() for p in parts for o in range(4) for s in (FORE, BACK)}
        threef = {(p, o): self.new() for p in parts for o in range(4)}
        core = {(p, a, b): self.new() for p in parts for a in range(4) for b in range(4)}

        def dims(p):
            return ORDERS[p]

        def at1(p, a):
            return self.moved(me, dims(p)[0], a)

        def at2(p, a, b):
            return self.moved(at1(p, a), dims(p)[1], b)

        def set3(p, b, c, k=None):
            d = dims(p)
            at = self.moved(self.moved(me, d[1], b), d[2], c)
            if k is not None:
                at = {**at, "k": k}
            return self.set_of(p, at, d[0])

        def to(p, i, s):
            return self.moved(me, dims(p)[i], s)

        def cross(p, b, c):
            self.copy(set3(p, b, c), core[p, b, c], self.other)

        for p in parts:
            for s in (FORE, BACK):
                self.copy(self.block(p, me), one[p, s], to(p, 0, s))
        for p in parts:
            for s in (FORE, BACK):
                self.copy(self.block(p, me), two[p, 0, s], to(p, 1, s))
        yield
        for p in parts:
            for s in (FORE, BACK):
                back = 4 - s
                self.arrived(self.block(p, at1(p, back)), one[p, s])
                self.copy(self.block(p, at1(p, back), half=0 if s == FORE else 1), onef[p, s], to(p, 0, s))
                for s2 in (FORE, BACK):
                    self.copy(self.block(p, at1(p, back)), two[p, back, s2], to(p, 1, s2))
        yield
        for p in parts:
            for s in (FORE, BACK):
                self.arrived(self.block(p, at1(p, 2), half=0 if s == FORE else 1), onef[p, s])
            for s2 in (FORE, BACK):
                self.copy(self.block(p, at1(p, 2)), two[p, 2, s2], to(p, 1, s2))
            for s3 in (FORE, BACK):
                self.copy(set3(p, 0, 0), three[p, 0, s3], to(p, 2, s3))
            cross(p, 0, 0)
        yield
        FIRST = {FORE: (0, 3), BACK: (1, 2)}
        for p in parts:
            for o in (0, 3, 1, 2):
                for s in (FORE, BACK):
                    back = 4 - s
                    self.arrived(self.block(p, at2(p, o, back)), two[p, o, s])
                    if o in FIRST[s]:
                        self.copy(self.block(p, at2(p, o, back)), twof[p, o], to(p, 1, s))
            for b in (3, 1):
                for s3 in (FORE, BACK):
                    self.copy(set3(p, b, 0), three[p, b, s3], to(p, 2, s3))
                cross(p, b, 0)
        yield
        for p in parts:
            for o in (0, 3, 1, 2):
                self.arrived(self.block(p, at2(p, o, 2)), twof[p, o])
            for s3 in (FORE, BACK):
                self.copy(set3(p, 2, 0), three[p, 2, s3], to(p, 2, s3))
            cross(p, 2, 0)
        for b in (0, 3, 1, 2):
            yield
            for p in parts:
                for s in (FORE, BACK):
                    back = 4 - s
                    self.arrived(set3(p, b, back), three[p, b, s])
                    if b in FIRST[s]:
                        self.copy(set3(p, b, back), threef[p, b], to(p, 2, s))
                    cross(p, b, back)
        yield
        for b in (0, 3, 1, 2):
            for p in parts:
                self.arrived(set3(p, b, 2), threef[p, b])
                cross(p, b, 2)
        for p in parts:
            for a in range(4):
                for b in range(4):
                    self.arrived(set3(p, a, b, k=self.other["k"]), core[p, a, b])
        for ref, n in self.sent:
            pltpu.make_async_remote_copy(ref, ref, self.send.at[n], self.recv.at[n], device_id=self.mine, device_id_type=MESH).wait_send()


def send_to(src, dst, ssem, rsem, to):
    c = pltpu.make_async_remote_copy(src, dst, ssem, rsem, device_id=to, device_id_type=MESH)
    c.start()
    return c


UB = 16
STEPS = 512 // UB
GRP = 256
PAD = 129


def spread_pair(at, pair, q_ref, p_ref, v_ref, dst):
    iq = lax.broadcasted_iota(jnp.int32, (128, 128), 0).astype(F32).astype(BF)
    ip = lax.broadcasted_iota(jnp.int32, (256, 128), 0).astype(F32).astype(BF)
    zero = jnp.zeros((128, 128), BF)

    def row(ref, b, n):
        one = jnp.broadcast_to(ref[pl.ds(b, 1), :], (16, 128)).astype(BF)
        return jnp.concatenate([one] * (n // 16), axis=0)

    qs, ps = [], []
    for j in range(2):
        b = at + 2 * pair + j
        qs.append(jnp.where(iq == row(q_ref, b, 128), row(v_ref, b, 128), zero))
        ps.append(jnp.where(ip == row(p_ref, b, 256), jnp.ones((), BF), jnp.zeros((), BF)))
    lhs = jnp.concatenate([jnp.concatenate([qs[0], zero], 1), jnp.concatenate([zero, qs[1]], 1)], 0)
    w = lax.dot_general(lhs, jnp.concatenate(ps, 1), NT, preferred_element_type=F32)
    for j in range(2):
        for h in range(2):
            dst[h, pl.ds((2 * pair + j) * PAD, 128), :] = w[j * 128:(j + 1) * 128, h * 128:(h + 1) * 128]


def split_rows(q, rows, src, whi, wlo):
    for h in range(2):
        f = src[h, pl.ds(q, UB, stride=PAD), :]
        hi = f.astype(BF)
        whi[q * 2 + h, rows, :] = hi
        wlo[q * 2 + h, rows, :] = (f - hi.astype(F32)).astype(BF)


def spread_split(at, rows, q_ref, p_ref, v_ref, src, dst, whi, wlo):
    for pair in range(UB // 2):
        spread_pair(at, pair, q_ref, p_ref, v_ref, dst)
        for q in range(pair * 16, pair * 16 + 16):
            split_rows(q, rows, src, whi, wlo)


def send_to(src, dst, ssem, rsem, to):
    c = pltpu.make_async_remote_copy(src, dst, ssem, rsem, device_id=to, device_id_type=MESH)
    c.start()
    return c


def take(ref, sem, me):
    pltpu.make_async_remote_copy(ref, ref, sem, sem, device_id=me, device_id_type=MESH).wait_recv()


def main_body(piece, spiece, q_ref, p_ref, v_ref, sec_ref, own_ref, out_ref, gt_ref, gs_ref, spill,
              t, s_vm, part, parts, wfa, wfb, whi, wlo, fold,
              send, recv, ssem, srecv, csem, crecv, gsem, grecv, psem, lsem, lose):
    r, c = lax.axis_index("rows"), lax.axis_index("cols")
    g = Gather(t, send, recv)
    me = g.me
    cp = pltpu.make_async_copy(piece, t.at[me["z"], me["x"], me["k"], me["y"]], lsem.at[0])
    cp.start()
    cs = pltpu.make_async_copy(spiece, s_vm.at[r], lsem.at[1])
    cs.start()
    sent = []

    def push(src, dst, ssem, rsem, n, to):
        send_to(src, dst, ssem.at[n], rsem.at[n], to)
        sent.append((src, ssem, n))

    cp.wait()
    run = g.run()
    next(run)
    for i in range(1, 16):
        push(spiece, s_vm.at[r], ssem, srecv, i - 1, (lax.rem(r + i, 16), c))
    cs.wait()

    mine = gs_ref.at[r]

    def second_gram():
        for i in range(1, 16):
            take(s_vm.at[lax.rem(r + 16 - i, 16)], srecv.at[i - 1], (r, c))
        chunk = lax.dot_general(s_vm[r], s_vm[...].reshape(256, 2048), NT, preferred_element_type=F32)
        part[...] = chunk
        parts[c] = chunk
        for i in range(1, 8):
            push(part, parts.at[c], csem, crecv, i - 1, (r, lax.rem(c + i, 8)))

    def second_gram_sum():
        for i in range(1, 8):
            take(parts.at[lax.rem(c + 8 - i, 8)], crecv.at[i - 1], (r, c))
        gs_ref[r] = sum(parts[i] for i in range(8))
        for i in range(1, 16):
            push(mine, mine, gsem, grecv, i - 1, (lax.rem(r + i, 16), c))

    def park(step):
        rows = pl.ds(pl.multiple_of(step * UB, UB), UB)
        return (
            pltpu.make_async_copy(whi.at[:, rows, :], spill.at[0, :, rows, :], psem.at[0, step]),
            pltpu.make_async_copy(wlo.at[:, rows, :], spill.at[1, :, rows, :], psem.at[1, step]),
        )

    todo = {j: [] for j in range(STEPS // 2)}
    for j in EVENTS:
        todo[j].append(lambda: next(run))
    todo[GRAM_AT].append(second_gram)
    todo[SUM_AT].append(second_gram_sum)

    def iteration(i, _):
        for j in range(STEPS // 2):
            if todo[j]:
                @pl.when(i == j)
                def _():
                    for f in todo[j]:
                        f()
        for half in range(2):
            step = lax.rem(2 * i + half + STEPS - 1, STEPS)
            slot = lax.rem(step, 16)

            @pl.when((step >= 16) & (2 * i + half >= 1))
            def _():
                for x in park(slot):
                    x.wait()

            rows = pl.ds(pl.multiple_of(slot * UB, UB), UB)
            at = pl.multiple_of((2 * i + half) * UB, UB)
            src, dst = ((wfb, wfa), (wfa, wfb))[half]
            spread_split(at, rows, q_ref, p_ref, v_ref, src, dst, whi, wlo)

            @pl.when(step < 16)
            def _():
                for x in park(slot):
                    x.start()
        return 0

    lax.fori_loop(0, STEPS // 2, iteration, 0)
    for x in park(15):
        x.wait()
    for q in range(128):
        split_rows(q, pl.ds(GRP - UB, UB), wfb, whi, wlo)
    for _ in run:
        pass

    def back(i):
        tiles = pl.ds(pl.multiple_of(i * 32, 32), 32)
        return (
            pltpu.make_async_copy(spill.at[0, tiles], whi.at[tiles], lose.at[0, i]),
            pltpu.make_async_copy(spill.at[1, tiles], wlo.at[tiles], lose.at[1, i]),
        )

    gt_ref[...] = jnp.zeros((256, 256), F32)
    fold[...] = jnp.zeros((512, 256), F32)
    for first in (True, False):
        def dense(i, _):
            if not first:
                for x in back(i):
                    x.wait()
            y, low = lax.div(i, 2), lax.rem(i, 2)
            tt = jnp.concatenate([t[low + 2 * h, :, :, y].reshape(128, 4096) for h in range(2)], 0)
            side = lambda w: jnp.concatenate([w[i * 32 + j] for j in range(32)], 1)
            lhs = jnp.concatenate([side(whi), side(wlo)] + ([tt] if first else []), 0)
            res = lax.dot_general(lhs, tt, NT, preferred_element_type=F32)
            fold[pl.ds(GRP if first else 0, GRP), :] += res[:GRP] + res[GRP:2 * GRP]
            if first:
                gt_ref[...] += res[2 * GRP:]
                for x in back(i):
                    x.start()
            return 0

        lax.fori_loop(0, 8, dense, 0)

    one, zero = jnp.ones((), BF), jnp.zeros((), BF)
    second = jnp.zeros((256, 512), F32)
    for j in range(4):
        ij = lax.broadcasted_iota(jnp.int32, (512, 512), 0) + j * 512
        pick = jnp.where(ij == sec_ref[...], one, zero)
        second += lax.dot_general(s_vm[:, :, j * 512:(j + 1) * 512].reshape(256, 512), pick, NN, preferred_element_type=F32)
    contrib = second * fold[...].T
    hi = contrib.astype(BF)
    rest = contrib - hi.astype(F32)
    mid = rest.astype(BF)
    low = (rest - mid.astype(F32)).astype(BF)
    lhs = jnp.concatenate([hi, mid, low], 0)
    for j in range(8):
        ii = lax.broadcasted_iota(jnp.int32, (128, 512), 0) + j * 128
        put = jnp.where(ii == own_ref[...], one, zero)
        res = lax.dot_general(lhs, put, NT, preferred_element_type=F32)
        out_ref[j] = res[:256] + (res[256:512] + res[512:])
    for i in range(1, 16):
        take(gs_ref.at[lax.rem(r + 16 - i, 16)], grecv.at[i - 1], (r, c))
    for ref, sem, n in sent:
        pltpu.make_async_remote_copy(ref, ref, sem.at[n], sem.at[n], device_id=(r, c), device_id_type=MESH).wait_send()


EVENTS = (1, 3, 5, 7, 9, 11, 13, 15)
GRAM_AT = 10
SUM_AT = 14


def main(piece, spiece, q, p, v, sec, own):
    D = pltpu.SemaphoreType.DMA
    return pl.pallas_call(
        main_body,
        out_shape=(
            jax.ShapeDtypeStruct((8, 256, 128), F32),
            jax.ShapeDtypeStruct((256, 256), F32),
            jax.ShapeDtypeStruct((16, 16, 256), F32),
            jax.ShapeDtypeStruct((2, 256, GRP, 128), BF),
        ),
        in_specs=[ANY, ANY] + [INV] * 5,
        out_specs=(INV, INV, INV, ANY),
        scratch_shapes=[
            VMEM((4, 4, 2, 4, 16, 4096), BF), VMEM((16, 16, 2048), BF), VMEM((16, 256), F32), VMEM((8, 16, 256), F32),
            VMEM((2, UB * PAD, 128), F32), VMEM((2, UB * PAD, 128), F32),
            VMEM((256, GRP, 128), BF), VMEM((256, GRP, 128), BF), VMEM((512, 256), F32),
            D((SEMS,)), D((SEMS,)), D((15,)), D((15,)), D((7,)), D((7,)), D((15,)), D((15,)), D((2, 16)), D((2,)), D((2, 8)),
        ],
        compiler_params=pltpu.CompilerParams(has_side_effects=True, vmem_limit_bytes=67043328),
        name="gather_spread_fold",
    )(piece, spiece, q, p, v, sec, own)


def inverse_body(gs_ref, gt_ref, out_ref, a_ref, x_ref):
    gram = (gs_ref[...].reshape(256, 256) / 16384) * (gt_ref[...] / 32768)
    eye = (lax.broadcasted_iota(jnp.int32, (256, 256), 0) == lax.broadcasted_iota(jnp.int32, (256, 256), 1)).astype(F32)
    diag = gram * eye
    down = 1 / jnp.sqrt(jnp.sum(diag, axis=1, keepdims=True))
    along = 1 / jnp.sqrt(jnp.sum(diag, axis=0, keepdims=True))
    a = gram * down * along
    a_ref[...] = a
    bound = jnp.max(jnp.sum(jnp.abs(a), axis=0))
    x_ref[...] = eye * (2 / (1 + bound))

    def dot(u, w):
        return lax.dot_general(u, w, NN, precision=HIGH, preferred_element_type=F32)

    def go(state):
        return (state[0] < 64) & (state[1] > 1e-4)

    def step(state):
        x = x_ref[...]
        rest = eye - dot(a_ref[...], x)
        x_ref[...] = x + dot(x, rest)
        return state[0] + 1, jnp.max(jnp.abs(rest))

    lax.while_loop(go, step, (0, jnp.float32(1.0)))
    out_ref[...] = x_ref[...] * down * along


def inverse(gs, gt):
    return pl.pallas_call(
        inverse_body,
        out_shape=jax.ShapeDtypeStruct((256, 256), F32),
        in_specs=[INV, INV],
        out_specs=INV,
        scratch_shapes=[VMEM((256, 256), F32), VMEM((256, 256), F32)],
        name="gram_inverse",
    )(gs, gt)


def k3_body(part, inv, out, got, x, rsem, rrecv, xsem, xrecv, lsem):
    r, c = lax.axis_index("rows"), lax.axis_index("cols")
    sent = []
    for i in range(1, 8):
        to = lax.rem(c + i, 8)
        sent.append(send_to(part.at[to], got.at[i - 1], rsem.at[i - 1], rrecv.at[i - 1], (r, to)))
    total = part[c]
    for i in range(7):
        pltpu.make_async_remote_copy(got.at[i], got.at[i], rsem.at[i], rrecv.at[i], device_id=(r, c), device_id_type=MESH).wait_recv()
        total = total + got[i]
    solved = lax.dot_general(inv[...], total, NN, precision=HIGH, preferred_element_type=F32)
    x[...] = solved.reshape(16, 16, 128)
    home = lax.div(r, 2)
    slot = lax.rem(r, 2) * 8 + c
    mine = home == c
    lanes = pl.ds(pl.multiple_of(slot * 128, 128), 128)
    for i in range(1, 16):
        to = lax.rem(r + i, 16)
        sent.append(send_to(x.at[to], out.at[:, lanes], xsem.at[i], xrecv.at[slot], (to, home)))

    near = pltpu.make_async_copy(x.at[r], out.at[:, lanes], lsem)
    far = pltpu.make_async_remote_copy(x.at[r], out.at[:, lanes], xsem.at[0], xrecv.at[slot], device_id=(r, home), device_id_type=MESH)

    @pl.when(mine)
    def _():
        near.start()

    @pl.when(jnp.logical_not(mine))
    def _():
        far.start()

    for i in range(16):
        there = out.at[:, pl.ds(i * 128, 128)]
        take = pltpu.make_async_remote_copy(there, there, xsem.at[0], xrecv.at[i], device_id=(r, c), device_id_type=MESH)

        @pl.when(jnp.logical_not(mine & (slot == i)))
        def _():
            take.wait_recv()

    @pl.when(mine)
    def _():
        near.wait()

    @pl.when(jnp.logical_not(mine))
    def _():
        far.wait_send()

    for s in sent:
        s.wait_send()


def k3(part, inv):
    D = pltpu.SemaphoreType.DMA
    return pl.pallas_call(
        k3_body,
        out_shape=jax.ShapeDtypeStruct((16, 2048), F32),
        in_specs=[INV, INV],
        out_specs=INV,
        scratch_shapes=[VMEM((7, 256, 128), F32), VMEM((16, 16, 128), F32), D((7,)), D((7,)), D((16,)), D((16,)), D(())],
        compiler_params=pltpu.CompilerParams(has_side_effects=True),
        name="reduce_solve_place",
    )(part, inv)


def per_device(values, length, owner, second, third, live_blocks, second_factor, third_factor):
    r, c = lax.axis_index("rows"), lax.axis_index("cols")
    lane = jnp.arange(128, dtype=jnp.int32)
    slot = jnp.arange(512, dtype=jnp.int32)
    live = (lane[None, :] < length[:, None]) & (slot < live_blocks[0])[:, None]
    v = jnp.where(live, values, jnp.zeros((), BF)).astype(F32)
    q = (third >> 8).astype(F32)
    p = (third & 255).astype(F32)
    sec = (second - c * 2048).reshape(1, 512)
    own = (owner - r * 1024).reshape(1, 512)
    part, gt, gs, _ = main(third_factor.T, second_factor.T, q, p, v, sec, own)
    inv = inverse(gs, gt)
    return k3(part, inv).T


def solution(mesh):
    both = P(("rows", "cols"))
    wide = P(("rows", "cols"), None)
    return jax.shard_map(
        per_device,
        mesh=mesh,
        in_specs=(wide, both, both, both, wide, both, P("cols", "rows"), P("cols", "rows")),
        out_specs=P("cols", "rows"),
        check_vma=False,
    )
```

```python
import jax
import jax.numpy as jnp
from jax import lax
from jax.experimental import pallas as pl
from jax.experimental.pallas import tpu as pltpu
from jax.sharding import PartitionSpec as P

F32 = jnp.float32
BF = jnp.bfloat16
MESH = pl.DeviceIdType.MESH
NT = (((1,), (1,)), ((), ()))
NN = (((1,), (0,)), ((), ()))
HIGH = lax.Precision.HIGHEST
VMEM = pltpu.VMEM
ANY = pl.BlockSpec(memory_space=pl.ANY)
INV = pl.BlockSpec(memory_space=pltpu.VMEM)

PARTS = ((0, 1152), (1152, 1408), (2560, 1536))
ORDERS = ("xyz", "yzx", "zxy")
SEMS = 28 * 3 + 16 * 3


def place():
    r, c = lax.axis_index("rows"), lax.axis_index("cols")
    return {"z": lax.div(r, 8) * 2 + lax.rem(c, 2), "x": lax.rem(lax.div(r, 2), 4), "k": lax.rem(r, 2), "y": lax.div(c, 2)}


def device(at):
    return (lax.div(at["z"], 2) * 8 + at["x"] * 2 + at["k"], at["y"] * 2 + lax.rem(at["z"], 2))


class Gather:
    def __init__(self, t, send, recv):
        self.t, self.send, self.recv = t, send, recv
        self.me = me = place()
        self.mine = device(me)
        self.steps = {d: [me[d], *(lax.rem(me[d] + i, 4) for i in (1, 2, 3))] for d in "zxy"}
        self.other = {**me, "k": 1 - me["k"]}
        self.used = 0
        self.sent = []

    def moved(self, at, dim, step):
        return {**at, dim: self.steps[dim][step]}

    def block(self, part, at, half=None):
        start, size = PARTS[part]
        if half is not None:
            first = (size // 128 // 2) * 128
            start, size = (start, first) if half == 0 else (start + first, size - first)
        return self.t.at[at["z"], at["x"], at["k"], at["y"], :, pl.ds(start, size)]

    def set_of(self, part, at, whole):
        start, size = PARTS[part]
        return self.t.at[*[slice(None) if d in whole else at[d] for d in "zxky"], :, pl.ds(start, size)]

    def new(self):
        self.used += 1
        return self.used - 1

    def copy(self, ref, n, to):
        c = pltpu.make_async_remote_copy(ref, ref, self.send.at[n], self.recv.at[n], device_id=device(to), device_id_type=MESH)
        c.start()
        self.sent.append((ref, n))

    def arrived(self, ref, n):
        pltpu.make_async_remote_copy(ref, ref, self.send.at[n], self.recv.at[n], device_id=self.mine, device_id_type=MESH).wait_recv()

    def run(self):
        me = self.me
        FORE, BACK = 1, 3
        parts = range(3)
        one = {(p, s): self.new() for p in parts for s in (FORE, BACK)}
        onef = {(p, s): self.new() for p in parts for s in (FORE, BACK)}
        two = {(p, o, s): self.new() for p in parts for o in range(4) for s in (FORE, BACK)}
        twof = {(p, o): self.new() for p in parts for o in range(4)}
        three = {(p, o, s): self.new() for p in parts for o in range(4) for s in (FORE, BACK)}
        threef = {(p, o): self.new() for p in parts for o in range(4)}
        core = {(p, a, b): self.new() for p in parts for a in range(4) for b in range(4)}

        def dims(p):
            return ORDERS[p]

        def at1(p, a):
            return self.moved(me, dims(p)[0], a)

        def at2(p, a, b):
            return self.moved(at1(p, a), dims(p)[1], b)

        def set3(p, b, c, k=None):
            d = dims(p)
            at = self.moved(self.moved(me, d[1], b), d[2], c)
            if k is not None:
                at = {**at, "k": k}
            return self.set_of(p, at, d[0])

        def to(p, i, s):
            return self.moved(me, dims(p)[i], s)

        def cross(p, b, c):
            self.copy(set3(p, b, c), core[p, b, c], self.other)

        for p in parts:
            for s in (FORE, BACK):
                self.copy(self.block(p, me), one[p, s], to(p, 0, s))
        for p in parts:
            for s in (FORE, BACK):
                self.copy(self.block(p, me), two[p, 0, s], to(p, 1, s))
        yield
        for p in parts:
            for s in (FORE, BACK):
                back = 4 - s
                self.arrived(self.block(p, at1(p, back)), one[p, s])
                self.copy(self.block(p, at1(p, back), half=0 if s == FORE else 1), onef[p, s], to(p, 0, s))
                for s2 in (FORE, BACK):
                    self.copy(self.block(p, at1(p, back)), two[p, back, s2], to(p, 1, s2))
        yield
        for p in parts:
            for s in (FORE, BACK):
                self.arrived(self.block(p, at1(p, 2), half=0 if s == FORE else 1), onef[p, s])
            for s2 in (FORE, BACK):
                self.copy(self.block(p, at1(p, 2)), two[p, 2, s2], to(p, 1, s2))
            for s3 in (FORE, BACK):
                self.copy(set3(p, 0, 0), three[p, 0, s3], to(p, 2, s3))
            cross(p, 0, 0)
        yield
        FIRST = {FORE: (0, 3), BACK: (1, 2)}
        for p in parts:
            for o in (0, 3, 1, 2):
                for s in (FORE, BACK):
                    back = 4 - s
                    self.arrived(self.block(p, at2(p, o, back)), two[p, o, s])
                    if o in FIRST[s]:
                        self.copy(self.block(p, at2(p, o, back)), twof[p, o], to(p, 1, s))
            for b in (3, 1):
                for s3 in (FORE, BACK):
                    self.copy(set3(p, b, 0), three[p, b, s3], to(p, 2, s3))
                cross(p, b, 0)
        yield
        for p in parts:
            for o in (0, 3, 1, 2):
                self.arrived(self.block(p, at2(p, o, 2)), twof[p, o])
            for s3 in (FORE, BACK):
                self.copy(set3(p, 2, 0), three[p, 2, s3], to(p, 2, s3))
            cross(p, 2, 0)
        for b in (0, 3, 1, 2):
            yield
            for p in parts:
                for s in (FORE, BACK):
                    back = 4 - s
                    self.arrived(set3(p, b, back), three[p, b, s])
                    if b in FIRST[s]:
                        self.copy(set3(p, b, back), threef[p, b], to(p, 2, s))
                    cross(p, b, back)
        yield
        for b in (0, 3, 1, 2):
            for p in parts:
                self.arrived(set3(p, b, 2), threef[p, b])
                cross(p, b, 2)
        for p in parts:
            for a in range(4):
                for b in range(4):
                    self.arrived(set3(p, a, b, k=self.other["k"]), core[p, a, b])
        for ref, n in self.sent:
            pltpu.make_async_remote_copy(ref, ref, self.send.at[n], self.recv.at[n], device_id=self.mine, device_id_type=MESH).wait_send()


def send_to(src, dst, ssem, rsem, to):
    c = pltpu.make_async_remote_copy(src, dst, ssem, rsem, device_id=to, device_id_type=MESH)
    c.start()
    return c


UB = 16
STEPS = 512 // UB
GRP = 256
PAD = 129


def spread_pair(at, pair, ins, dst):
    third_ref, value_ref, length_ref, live_ref = ins
    lane = lax.broadcasted_iota(jnp.int32, (16, 128), 1)
    iq = lax.broadcasted_iota(jnp.int32, (128, 128), 0).astype(F32).astype(BF)
    ip = lax.broadcasted_iota(jnp.int32, (256, 128), 0).astype(F32).astype(BF)
    zero = jnp.zeros((128, 128), BF)

    def wide(one, n):
        return jnp.concatenate([one] * (n // 16), axis=0)

    qs, ps = [], []
    for j in range(2):
        b = at + 2 * pair + j
        third = jnp.broadcast_to(third_ref[pl.ds(b, 1), :], (16, 128))
        value = jnp.broadcast_to(value_ref[pl.ds(b, 1), :], (16, 128))
        used = jnp.where(b < live_ref[0], length_ref[b], 0)
        value = wide(jnp.where(lane < used, value, 0.0).astype(BF), 128)
        high = wide((third >> 8).astype(F32).astype(BF), 128)
        low = wide((third & 255).astype(F32).astype(BF), 256)
        qs.append(jnp.where(iq == high, value, zero))
        ps.append(jnp.where(ip == low, jnp.ones((), BF), jnp.zeros((), BF)))
    lhs = jnp.concatenate([jnp.concatenate([qs[0], zero], 1), jnp.concatenate([zero, qs[1]], 1)], 0)
    w = lax.dot_general(lhs, jnp.concatenate(ps, 1), NT, preferred_element_type=F32)
    for j in range(2):
        for h in range(2):
            dst[h, pl.ds((2 * pair + j) * PAD, 128), :] = w[j * 128:(j + 1) * 128, h * 128:(h + 1) * 128]


def split_rows(q, rows, src, whi, wlo):
    for h in range(2):
        f = src[h, pl.ds(q, UB, stride=PAD), :]
        hi = f.astype(BF)
        whi[q * 2 + h, rows, :] = hi
        wlo[q * 2 + h, rows, :] = (f - hi.astype(F32)).astype(BF)


def spread_split(at, rows, ins, src, dst, whi, wlo):
    for pair in range(UB // 2):
        spread_pair(at, pair, ins, dst)
        for q in range(pair * 16, pair * 16 + 16):
            split_rows(q, rows, src, whi, wlo)


def send_to(src, dst, ssem, rsem, to):
    c = pltpu.make_async_remote_copy(src, dst, ssem, rsem, device_id=to, device_id_type=MESH)
    c.start()
    return c


def take(ref, sem, me):
    pltpu.make_async_remote_copy(ref, ref, sem, sem, device_id=me, device_id_type=MESH).wait_recv()


def main_body(piece, spiece, third_ref, values_ref, length_ref, live_ref, sec_ref, own_ref, out, spill,
              t, s_vm, near, far, part, parts, wfa, wfb, whi, wlo, fold, value_ref, gt_ref, gs_ref, total, got, a_ref, x_ref, answer,
              send, recv, ssem, srecv, csem, crecv, gsem, grecv, psem, lsem, lose, rsem, rrecv, xsem, xrecv):
    r, c = lax.axis_index("rows"), lax.axis_index("cols")
    g = Gather(t, send, recv)
    me = g.me
    cp = pltpu.make_async_copy(piece, t.at[me["z"], me["x"], me["k"], me["y"]], lsem.at[0])
    cp.start()
    cs = pltpu.make_async_copy(spiece, s_vm.at[lax.div(me["z"], 2), me["x"], me["k"]], lsem.at[1])
    cs.start()
    peers = [(lax.rem(r + i, 16), c) for i in range(1, 16)] + [(r, lax.rem(c + i, 8)) for i in range(1, 8)]
    peers += [device(g.moved(me, "z", 1)), device(g.moved(me, "z", 3))]
    barrier = pltpu.get_barrier_semaphore()
    for to in peers:
        pl.semaphore_signal(barrier, inc=1, device_id=to, device_id_type=MESH)
    home = lax.div(r, 2)
    at_home = home == c
    for i in range(16):
        source = (2 * c + i // 8, i % 8)

        @pl.when(jnp.logical_not((source[0] == r) & (c == source[1])))
        def _():
            pl.semaphore_signal(barrier, inc=1, device_id=source, device_id_type=MESH)
    value_ref[...] = values_ref[...].astype(F32)
    ins = (third_ref, value_ref, length_ref, live_ref)
    pl.semaphore_wait(barrier, 40 - at_home.astype(jnp.int32))
    sent = []

    def push(src, dst, ssem, rsem, n, to):
        send_to(src, dst, ssem.at[n], rsem.at[n], to)
        sent.append((lambda: src, ssem, n))

    cp.wait()
    run = g.run()
    next(run)
    cs.wait()
    FORE, BACK = 1, 3
    relay = {FORE: near, BACK: far}

    def hop(src, dst, n, to):
        send_to(src(), dst(), ssem.at[n], srecv.at[n], device(to))
        sent.append((src, ssem, n))

    xs = g.steps["x"]
    zs = [lax.div(z, 2) for z in g.steps["z"]]

    def plane(z, x=None, half=None):
        ref = s_vm.at[zs[z], slice(None) if x is None else xs[x], me["k"]]
        return ref if half is None else ref.at[:, pl.ds(half * 1024, 1024)]

    def stop(way, j):
        return relay[way].at[j]

    for n, way in enumerate((FORE, BACK)):
        hop(lambda: plane(0, 0), lambda: plane(0, 0), n, g.moved(me, "x", way))

    def second_one():
        for n, way in enumerate((FORE, BACK)):
            take(plane(0, 4 - way), srecv.at[n], (r, c))
            half = lambda n=n, way=way: plane(0, 4 - way, half=n)
            hop(half, half, 2 + n, g.moved(me, "x", way))

    def second_two():
        for n, way in enumerate((FORE, BACK)):
            take(plane(0, 2, half=n), srecv.at[2 + n], (r, c))
        for n, way in enumerate((FORE, BACK)):
            for j in range(2):
                hop(lambda n=n, j=j: plane(0, 2 * n + j), lambda: stop(way, j), 4 + 2 * n + j, g.moved(me, "z", way))
        hop(lambda: plane(0), lambda: plane(0), 12, g.other)

    def second_three():
        for n, way in enumerate((FORE, BACK)):
            for j in range(2):
                take(stop(way, j), srecv.at[4 + 2 * n + j], (r, c))
                hop(lambda way=way, j=j: stop(way, j), lambda: plane(4 - way, 2 * n + j), 8 + 2 * n + j, g.moved(me, "z", way))

    def second_four():
        for n in range(2):
            for j in range(2):
                take(plane(2, 2 * n + j), srecv.at[8 + 2 * n + j], (r, c))
        hop(lambda: plane(2), lambda: plane(2), 13, g.other)

    mine = gs_ref.at[r]

    def second_gram():
        for n, z in ((12, 0), (13, 2)):
            take(s_vm.at[zs[z], :, g.other["k"]], srecv.at[n], (r, c))
        chunk = lax.dot_general(s_vm[zs[0], me["x"], me["k"]], s_vm[...].reshape(256, 2048), NT, preferred_element_type=F32)
        part[...] = chunk
        parts[c] = chunk
        for i in range(1, 8):
            push(part, parts.at[c], csem, crecv, i - 1, (r, lax.rem(c + i, 8)))

    def second_gram_sum():
        for i in range(1, 8):
            take(parts.at[lax.rem(c + 8 - i, 8)], crecv.at[i - 1], (r, c))
        gs_ref[r] = sum(parts[i] for i in range(8))
        for i in range(1, 16):
            push(mine, mine, gsem, grecv, i - 1, (lax.rem(r + i, 16), c))

    def park(step):
        rows = pl.ds(pl.multiple_of(step * UB, UB), UB)
        return (
            pltpu.make_async_copy(whi.at[:, rows, :], spill.at[0, :, rows, :], psem.at[0, step]),
            pltpu.make_async_copy(wlo.at[:, rows, :], spill.at[1, :, rows, :], psem.at[1, step]),
        )

    todo = {j: [] for j in range(STEPS // 2)}
    for j in EVENTS:
        todo[j].append(lambda: next(run))
    for j, f in zip(SECOND_AT, (second_one, second_two, second_three, second_four, second_gram, second_gram_sum)):
        todo[j].append(f)

    def iteration(i, _):
        for j in range(STEPS // 2):
            if todo[j]:
                @pl.when(i == j)
                def _():
                    for f in todo[j]:
                        f()
        for half in range(2):
            step = lax.rem(2 * i + half + STEPS - 1, STEPS)
            slot = lax.rem(step, 16)

            @pl.when((step >= 16) & (2 * i + half >= 1))
            def _():
                for x in park(slot):
                    x.wait()

            rows = pl.ds(pl.multiple_of(slot * UB, UB), UB)
            at = pl.multiple_of((2 * i + half) * UB, UB)
            src, dst = ((wfb, wfa), (wfa, wfb))[half]
            spread_split(at, rows, ins, src, dst, whi, wlo)

            @pl.when(step < 16)
            def _():
                for x in park(slot):
                    x.start()
        return 0

    lax.fori_loop(0, STEPS // 2, iteration, 0)
    for x in park(15):
        x.wait()
    for q in range(128):
        split_rows(q, pl.ds(GRP - UB, UB), wfb, whi, wlo)
    for _ in run:
        pass

    def back(i):
        tiles = pl.ds(pl.multiple_of(i * 32, 32), 32)
        return (
            pltpu.make_async_copy(spill.at[0, tiles], whi.at[tiles], lose.at[0, i]),
            pltpu.make_async_copy(spill.at[1, tiles], wlo.at[tiles], lose.at[1, i]),
        )

    gt_ref[...] = jnp.zeros((256, 256), F32)
    fold[...] = jnp.zeros((512, 256), F32)
    for first in (True, False):
        def dense(i, _):
            if not first:
                for x in back(i):
                    x.wait()
            y, low = lax.div(i, 2), lax.rem(i, 2)
            tt = jnp.concatenate([t[low + 2 * h, :, :, y].reshape(128, 4096) for h in range(2)], 0)
            side = lambda w: jnp.concatenate([w[i * 32 + j] for j in range(32)], 1)
            lhs = jnp.concatenate([side(whi), side(wlo)] + ([tt] if first else []), 0)
            res = lax.dot_general(lhs, tt, NT, preferred_element_type=F32)
            fold[pl.ds(GRP if first else 0, GRP), :] += res[:GRP] + res[GRP:2 * GRP]
            if first:
                gt_ref[...] += res[2 * GRP:]
                for x in back(i):
                    x.start()
            return 0

        lax.fori_loop(0, 8, dense, 0)

    one, zero = jnp.ones((), BF), jnp.zeros((), BF)
    second = jnp.zeros((256, 512), F32)
    for j in range(4):
        ij = lax.broadcasted_iota(jnp.int32, (512, 512), 0) + j * 512
        pick = jnp.where(ij == sec_ref[...] - c * 2048, one, zero)
        second += lax.dot_general(s_vm[:, :, :, :, j * 512:(j + 1) * 512].reshape(256, 512), pick, NN, preferred_element_type=F32)
    contrib = second * fold[...].T
    hi = contrib.astype(BF)
    lhs = jnp.concatenate([hi, (contrib - hi.astype(F32)).astype(BF)], 0)
    for j in range(4):
        ii = lax.broadcasted_iota(jnp.int32, (256, 512), 0) + j * 256
        put = jnp.where(ii == own_ref[...] - r * 1024, one, zero)
        res = lax.dot_general(lhs, put, NT, preferred_element_type=F32)
        both = res[:256] + res[256:]
        for h in range(2):
            total[2 * j + h] = both[:, h * 128:(h + 1) * 128]
    for i in range(1, 8):
        to = lax.rem(c + i, 8)
        send_to(total.at[to], got.at[i - 1], rsem.at[i - 1], rrecv.at[i - 1], (r, to))

    for i in range(1, 16):
        take(gs_ref.at[lax.rem(r + 16 - i, 16)], grecv.at[i - 1], (r, c))
    invert(gs_ref, gt_ref, a_ref, x_ref)
    rows = total[c]
    for i in range(7):
        take(got.at[i], rrecv.at[i], (r, c))
        rows = rows + got[i]
    answer[...] = lax.dot_general(a_ref[...], rows, NN, precision=HIGH, preferred_element_type=F32).reshape(16, 16, 128)

    slot = lax.rem(r, 2) * 8 + c
    lanes = pl.ds(pl.multiple_of(slot * 128, 128), 128)
    for i in range(1, 16):
        to = lax.rem(r + i, 16)
        send_to(answer.at[to], out.at[:, lanes], xsem.at[i], xrecv.at[slot], (to, home))
    here = pltpu.make_async_copy(answer.at[r], out.at[:, lanes], lsem.at[0])
    away = pltpu.make_async_remote_copy(answer.at[r], out.at[:, lanes], xsem.at[0], xrecv.at[slot], device_id=(r, home), device_id_type=MESH)

    @pl.when(at_home)
    def _():
        here.start()

    @pl.when(jnp.logical_not(at_home))
    def _():
        away.start()

    for make, sem, n in sent:
        ref = make()
        pltpu.make_async_remote_copy(ref, ref, sem.at[n], sem.at[n], device_id=(r, c), device_id_type=MESH).wait_send()
    for i in range(1, 8):
        pltpu.make_async_remote_copy(got.at[i - 1], got.at[i - 1], rsem.at[i - 1], rrecv.at[i - 1], device_id=(r, c), device_id_type=MESH).wait_send()
    for i in range(16):
        there = out.at[:, pl.ds(i * 128, 128)]

        @pl.when(jnp.logical_not(at_home & (slot == i)))
        def _():
            take(there, xrecv.at[i], (r, c))

    @pl.when(at_home)
    def _():
        here.wait()

    @pl.when(jnp.logical_not(at_home))
    def _():
        away.wait_send()

    for i in range(1, 16):
        pltpu.make_async_remote_copy(answer.at[0], answer.at[0], xsem.at[i], xrecv.at[0], device_id=(r, c), device_id_type=MESH).wait_send()


def invert(gs_ref, gt_ref, a_ref, x_ref):
    gram = (gs_ref[...].reshape(256, 256) / 16384) * (gt_ref[...] / 32768)
    eye = (lax.broadcasted_iota(jnp.int32, (256, 256), 0) == lax.broadcasted_iota(jnp.int32, (256, 256), 1)).astype(F32)
    diag = gram * eye
    down = 1 / jnp.sqrt(jnp.sum(diag, axis=1, keepdims=True))
    along = 1 / jnp.sqrt(jnp.sum(diag, axis=0, keepdims=True))
    a = gram * down * along
    a_ref[...] = a
    bound = jnp.max(jnp.sum(jnp.abs(a), axis=0, keepdims=True), axis=1, keepdims=True)
    x_ref[...] = eye * (2 / (1 + bound))

    def dot(u, w):
        return lax.dot_general(u, w, NN, precision=HIGH, preferred_element_type=F32)

    def step(i, _):
        now = x_ref[...]
        x_ref[...] = now + dot(now, eye - dot(a_ref[...], now))
        return 0

    lax.fori_loop(0, NEWTON, step, 0)
    a_ref[...] = x_ref[...] * down * along


NEWTON = 24
EVENTS = (1, 3, 5, 7, 9, 11, 13, 15)
SECOND_AT = (1, 3, 5, 8, 10, 14)


def main(piece, spiece, third, values, length, live, sec, own):
    D = pltpu.SemaphoreType.DMA
    smem = pl.BlockSpec(memory_space=pltpu.SMEM)
    return pl.pallas_call(
        main_body,
        out_shape=(jax.ShapeDtypeStruct((16, 2048), F32), jax.ShapeDtypeStruct((2, 256, GRP, 128), BF)),
        in_specs=[ANY, ANY, INV, INV, smem, smem, INV, INV],
        out_specs=(INV, ANY),
        scratch_shapes=[
            VMEM((4, 4, 2, 4, 16, 4096), BF), VMEM((2, 4, 2, 16, 2048), BF), VMEM((2, 16, 2048), BF), VMEM((2, 16, 2048), BF),
            VMEM((16, 256), F32), VMEM((8, 16, 256), F32),
            VMEM((2, UB * PAD, 128), F32), VMEM((2, UB * PAD, 128), F32),
            VMEM((256, GRP, 128), BF), VMEM((256, GRP, 128), BF), VMEM((512, 256), F32), VMEM((512, 128), F32),
            VMEM((256, 256), F32), VMEM((16, 16, 256), F32), VMEM((8, 256, 128), F32), VMEM((7, 256, 128), F32),
            VMEM((256, 256), F32), VMEM((256, 256), F32), VMEM((16, 16, 128), F32),
            D((SEMS,)), D((SEMS,)), D((14,)), D((14,)), D((7,)), D((7,)), D((15,)), D((15,)), D((2, 16)), D((2,)), D((2, 8)),
            D((7,)), D((7,)), D((16,)), D((16,)),
        ],
        compiler_params=pltpu.CompilerParams(has_side_effects=True, vmem_limit_bytes=67043328, collective_id=0),
        name="factor_update",
    )(piece, spiece, third, values, length, live, sec, own)


def per_device(values, length, owner, second, third, live_blocks, second_factor, third_factor):
    out, _ = main(third_factor.T, second_factor.T, third, values, length, live_blocks, second.reshape(1, 512), owner.reshape(1, 512))
    return out.T


def solution(mesh):
    both = P(("rows", "cols"))
    wide = P(("rows", "cols"), None)
    return jax.shard_map(
        per_device,
        mesh=mesh,
        in_specs=(wide, both, both, both, wide, both, P("cols", "rows"), P("cols", "rows")),
        out_specs=P("cols", "rows"),
        check_vma=False,
    )
```

```python
import jax
import jax.numpy as jnp
from jax import lax
from jax.experimental import pallas as pl
from jax.experimental.pallas import tpu as pltpu
from jax.sharding import PartitionSpec as P

F32 = jnp.float32
BF = jnp.bfloat16
MESH = pl.DeviceIdType.MESH
NT = (((1,), (1,)), ((), ()))
NN = (((1,), (0,)), ((), ()))
HIGH = lax.Precision.HIGHEST
VMEM = pltpu.VMEM
ANY = pl.BlockSpec(memory_space=pl.ANY)
INV = pl.BlockSpec(memory_space=pltpu.VMEM)

PARTS = ((0, 1152), (1152, 1408), (2560, 1536))
ORDERS = ("xyz", "yzx", "zxy")
SEMS = 52 * 3 + 16 * 3


def place():
    r, c = lax.axis_index("rows"), lax.axis_index("cols")
    return {"z": lax.div(r, 8) * 2 + lax.rem(c, 2), "x": lax.rem(lax.div(r, 2), 4), "k": lax.rem(r, 2), "y": lax.div(c, 2)}


def device(at):
    return (lax.div(at["z"], 2) * 8 + at["x"] * 2 + at["k"], at["y"] * 2 + lax.rem(at["z"], 2))


class Gather:
    def __init__(self, t, send, recv):
        self.t, self.send, self.recv = t, send, recv
        self.me = me = place()
        self.mine = device(me)
        self.steps = {d: [me[d], *(lax.rem(me[d] + i, 4) for i in (1, 2, 3))] for d in "zxy"}
        self.other = {**me, "k": 1 - me["k"]}
        self.used = 0
        self.sent = []

    def moved(self, at, dim, step):
        return {**at, dim: self.steps[dim][step]}

    def block(self, part, at, half=None):
        start, size = PARTS[part]
        if half is not None:
            first = (size // 128 // 2) * 128
            start, size = (start, first) if half == 0 else (start + first, size - first)
        return self.t.at[at["z"], at["x"], at["k"], at["y"], :, pl.ds(start, size)]

    def set_of(self, part, at, whole):
        start, size = PARTS[part]
        return self.t.at[*[slice(None) if d in whole else at[d] for d in "zxky"], :, pl.ds(start, size)]

    def new(self):
        self.used += 1
        return self.used - 1

    def copy(self, ref, n, to):
        c = pltpu.make_async_remote_copy(ref, ref, self.send.at[n], self.recv.at[n], device_id=device(to), device_id_type=MESH)
        c.start()
        self.sent.append((ref, n))

    def arrived(self, ref, n):
        pltpu.make_async_remote_copy(ref, ref, self.send.at[n], self.recv.at[n], device_id=self.mine, device_id_type=MESH).wait_recv()

    def run(self):
        me = self.me
        FORE, BACK = 1, 3
        parts = range(3)
        one = {(p, s): self.new() for p in parts for s in (FORE, BACK)}
        onef = {(p, s): self.new() for p in parts for s in (FORE, BACK)}
        two = {(p, o, s): self.new() for p in parts for o in range(4) for s in (FORE, BACK)}
        twof = {(p, o): self.new() for p in parts for o in range(4)}
        three = {(p, a, b, s): self.new() for p in parts for a in range(4) for b in range(4) for s in (FORE, BACK)}
        threef = {(p, o): self.new() for p in parts for o in range(4)}
        core = {(p, a, b): self.new() for p in parts for a in range(4) for b in range(4)}

        def dims(p):
            return ORDERS[p]

        def at1(p, a):
            return self.moved(me, dims(p)[0], a)

        def at2(p, a, b):
            return self.moved(at1(p, a), dims(p)[1], b)

        def set3(p, b, c, k=None):
            d = dims(p)
            at = self.moved(self.moved(me, d[1], b), d[2], c)
            if k is not None:
                at = {**at, "k": k}
            return self.set_of(p, at, d[0])

        def to(p, i, s):
            return self.moved(me, dims(p)[i], s)

        def cross(p, b, c):
            self.copy(set3(p, b, c), core[p, b, c], self.other)

        def third(p, a, b):
            for s3 in (FORE, BACK):
                self.copy(self.block(p, at2(p, a, b)), three[p, a, b, s3], to(p, 2, s3))

        for p in parts:
            for s in (FORE, BACK):
                self.copy(self.block(p, me), one[p, s], to(p, 0, s))
        for p in parts:
            for s in (FORE, BACK):
                self.copy(self.block(p, me), two[p, 0, s], to(p, 1, s))
        for p in parts:
            third(p, 0, 0)
        yield
        for p in parts:
            for s in (FORE, BACK):
                back = 4 - s
                self.arrived(self.block(p, at1(p, back)), one[p, s])
                self.copy(self.block(p, at1(p, back), half=0 if s == FORE else 1), onef[p, s], to(p, 0, s))
                for s2 in (FORE, BACK):
                    self.copy(self.block(p, at1(p, back)), two[p, back, s2], to(p, 1, s2))
                third(p, back, 0)
        yield
        for p in parts:
            for s in (FORE, BACK):
                self.arrived(self.block(p, at1(p, 2), half=0 if s == FORE else 1), onef[p, s])
            for s2 in (FORE, BACK):
                self.copy(self.block(p, at1(p, 2)), two[p, 2, s2], to(p, 1, s2))
            third(p, 2, 0)
            cross(p, 0, 0)
        yield
        FIRST = {FORE: (0, 3), BACK: (1, 2)}
        for o in (0, 3, 1, 2):
            for p in parts:
                for s in (FORE, BACK):
                    back = 4 - s
                    self.arrived(self.block(p, at2(p, o, back)), two[p, o, s])
                    if o in FIRST[s]:
                        self.copy(self.block(p, at2(p, o, back)), twof[p, o], to(p, 1, s))
                    third(p, o, back)
        for p in parts:
            for b in (3, 1):
                cross(p, b, 0)
        yield
        for p in parts:
            for o in (0, 3, 1, 2):
                self.arrived(self.block(p, at2(p, o, 2)), twof[p, o])
                third(p, o, 2)
            cross(p, 2, 0)
        for b in (0, 3, 1, 2):
            yield
            for p in parts:
                for s in (FORE, BACK):
                    back = 4 - s
                    for o in range(4):
                        self.arrived(self.block(p, self.moved(at2(p, o, b), dims(p)[2], back)), three[p, o, b, s])
                    if b in FIRST[s]:
                        self.copy(set3(p, b, back), threef[p, b], to(p, 2, s))
                    cross(p, b, back)
        yield
        for b in (0, 3, 1, 2):
            for p in parts:
                self.arrived(set3(p, b, 2), threef[p, b])
                cross(p, b, 2)
        for p in parts:
            for a in range(4):
                for b in range(4):
                    self.arrived(set3(p, a, b, k=self.other["k"]), core[p, a, b])
        for ref, n in self.sent:
            pltpu.make_async_remote_copy(ref, ref, self.send.at[n], self.recv.at[n], device_id=self.mine, device_id_type=MESH).wait_send()


def send_to(src, dst, ssem, rsem, to):
    c = pltpu.make_async_remote_copy(src, dst, ssem, rsem, device_id=to, device_id_type=MESH)
    c.start()
    return c


UB = 16
STEPS = 512 // UB
GRP = 256
PAD = 129


def spread_pair(at, pair, ins, dst):
    third_ref, value_ref, length_ref, live_ref = ins
    lane = lax.broadcasted_iota(jnp.int32, (16, 128), 1)
    iq = lax.broadcasted_iota(jnp.int32, (128, 128), 0).astype(F32).astype(BF)
    ip = lax.broadcasted_iota(jnp.int32, (256, 128), 0).astype(F32).astype(BF)
    zero = jnp.zeros((128, 128), BF)

    def wide(one, n):
        return jnp.concatenate([one] * (n // 16), axis=0)

    qs, ps = [], []
    for j in range(2):
        b = at + 2 * pair + j
        third = jnp.broadcast_to(third_ref[pl.ds(b, 1), :], (16, 128))
        value = jnp.broadcast_to(value_ref[pl.ds(b, 1), :], (16, 128))
        used = jnp.where(b < live_ref[0], length_ref[b], 0)
        value = wide(jnp.where(lane < used, value, 0.0).astype(BF), 128)
        high = wide((third >> 8).astype(F32).astype(BF), 128)
        low = wide((third & 255).astype(F32).astype(BF), 256)
        qs.append(jnp.where(iq == high, value, zero))
        ps.append(jnp.where(ip == low, jnp.ones((), BF), jnp.zeros((), BF)))
    lhs = jnp.concatenate([jnp.concatenate([qs[0], zero], 1), jnp.concatenate([zero, qs[1]], 1)], 0)
    w = lax.dot_general(lhs, jnp.concatenate(ps, 1), NT, preferred_element_type=F32)
    for j in range(2):
        for h in range(2):
            dst[h, pl.ds((2 * pair + j) * PAD, 128), :] = w[j * 128:(j + 1) * 128, h * 128:(h + 1) * 128]


def split_rows(q, rows, src, whi, wlo):
    for h in range(2):
        f = src[h, pl.ds(q, UB, stride=PAD), :]
        hi = f.astype(BF)
        whi[q * 2 + h, rows, :] = hi
        wlo[q * 2 + h, rows, :] = (f - hi.astype(F32)).astype(BF)


def spread_split(at, rows, ins, src, dst, whi, wlo):
    for pair in range(UB // 2):
        spread_pair(at, pair, ins, dst)
        for q in range(pair * 16, pair * 16 + 16):
            split_rows(q, rows, src, whi, wlo)


def send_to(src, dst, ssem, rsem, to):
    c = pltpu.make_async_remote_copy(src, dst, ssem, rsem, device_id=to, device_id_type=MESH)
    c.start()
    return c


def take(ref, sem, me):
    pltpu.make_async_remote_copy(ref, ref, sem, sem, device_id=me, device_id_type=MESH).wait_recv()


def main_body(piece, spiece, third_ref, values_ref, length_ref, live_ref, sec_ref, own_ref, out, spill,
              t, s_vm, near, far, part, parts, wfa, wfb, whi, wlo, fold, value_ref, gt_ref, gs_ref, total, got, a_ref, x_ref, r_ref, part3, parts3, answer,
              send, recv, ssem, srecv, csem, crecv, gsem, grecv, psem, lsem, lose, rsem, rrecv, xsem, xrecv, csem3, crecv3, gsem3, grecv3):
    r, c = lax.axis_index("rows"), lax.axis_index("cols")
    g = Gather(t, send, recv)
    me = g.me
    cp = pltpu.make_async_copy(piece, t.at[me["z"], me["x"], me["k"], me["y"]], lsem.at[0])
    cp.start()
    cs = pltpu.make_async_copy(spiece, s_vm.at[lax.div(me["z"], 2), me["x"], me["k"]], lsem.at[1])
    cs.start()
    peers = [(lax.rem(r + i, 16), c) for i in range(1, 16)] + [(r, lax.rem(c + i, 8)) for i in range(1, 8)]
    peers += [device(g.moved(me, "z", 1)), device(g.moved(me, "z", 3))]
    barrier = pltpu.get_barrier_semaphore()
    for to in peers:
        pl.semaphore_signal(barrier, inc=1, device_id=to, device_id_type=MESH)
    home = lax.div(r, 2)
    at_home = home == c
    for i in range(16):
        source = (2 * c + i // 8, i % 8)

        @pl.when(jnp.logical_not((source[0] == r) & (c == source[1])))
        def _():
            pl.semaphore_signal(barrier, inc=1, device_id=source, device_id_type=MESH)
    value_ref[...] = values_ref[...].astype(F32)
    ins = (third_ref, value_ref, length_ref, live_ref)
    pl.semaphore_wait(barrier, 40 - at_home.astype(jnp.int32))
    sent = []

    def push(src, dst, ssem, rsem, n, to):
        send_to(src, dst, ssem.at[n], rsem.at[n], to)
        sent.append((lambda: src, ssem, n))

    cp.wait()
    run = g.run()
    next(run)
    cs.wait()
    FORE, BACK = 1, 3
    relay = {FORE: near, BACK: far}

    def hop(src, dst, n, to):
        send_to(src(), dst(), ssem.at[n], srecv.at[n], device(to))
        sent.append((src, ssem, n))

    xs = g.steps["x"]
    zs = [lax.div(z, 2) for z in g.steps["z"]]

    def plane(z, x=None, half=None):
        ref = s_vm.at[zs[z], slice(None) if x is None else xs[x], me["k"]]
        return ref if half is None else ref.at[:, pl.ds(half * 1024, 1024)]

    def stop(way, j):
        return relay[way].at[j]

    for n, way in enumerate((FORE, BACK)):
        hop(lambda: plane(0, 0), lambda: plane(0, 0), n, g.moved(me, "x", way))

    def second_one():
        for n, way in enumerate((FORE, BACK)):
            take(plane(0, 4 - way), srecv.at[n], (r, c))
            half = lambda n=n, way=way: plane(0, 4 - way, half=n)
            hop(half, half, 2 + n, g.moved(me, "x", way))

    def second_two():
        for n, way in enumerate((FORE, BACK)):
            take(plane(0, 2, half=n), srecv.at[2 + n], (r, c))
        for n, way in enumerate((FORE, BACK)):
            for j in range(2):
                hop(lambda n=n, j=j: plane(0, 2 * n + j), lambda: stop(way, j), 4 + 2 * n + j, g.moved(me, "z", way))
        hop(lambda: plane(0), lambda: plane(0), 12, g.other)

    def second_three():
        for n, way in enumerate((FORE, BACK)):
            for j in range(2):
                take(stop(way, j), srecv.at[4 + 2 * n + j], (r, c))
                hop(lambda way=way, j=j: stop(way, j), lambda: plane(4 - way, 2 * n + j), 8 + 2 * n + j, g.moved(me, "z", way))

    def second_four():
        for n in range(2):
            for j in range(2):
                take(plane(2, 2 * n + j), srecv.at[8 + 2 * n + j], (r, c))
        hop(lambda: plane(2), lambda: plane(2), 13, g.other)

    mine = gs_ref.at[r]

    mine3 = gt_ref.at[r]

    def third_gram():
        y, low = me["y"], lax.rem(me["z"], 2)
        whole = jnp.concatenate([t[low + 2 * h, :, :, y].reshape(128, 4096) for h in range(2)], 0)
        chunk = lax.dot_general(t[me["z"], me["x"], me["k"], y], whole, NT, preferred_element_type=F32)
        part3[...] = chunk
        parts3[c] = chunk
        for i in range(1, 8):
            push(part3, parts3.at[c], csem3, crecv3, i - 1, (r, lax.rem(c + i, 8)))

    def third_gram_sum():
        for i in range(1, 8):
            take(parts3.at[lax.rem(c + 8 - i, 8)], crecv3.at[i - 1], (r, c))
        gt_ref[r] = sum(parts3[i] for i in range(8))
        for i in range(1, 16):
            push(mine3, mine3, gsem3, grecv3, i - 1, (lax.rem(r + i, 16), c))

    def second_gram():
        for n, z in ((12, 0), (13, 2)):
            take(s_vm.at[zs[z], :, g.other["k"]], srecv.at[n], (r, c))
        chunk = lax.dot_general(s_vm[zs[0], me["x"], me["k"]], s_vm[...].reshape(256, 2048), NT, preferred_element_type=F32)
        part[...] = chunk
        parts[c] = chunk
        for i in range(1, 8):
            push(part, parts.at[c], csem, crecv, i - 1, (r, lax.rem(c + i, 8)))

    def second_gram_sum():
        for i in range(1, 8):
            take(parts.at[lax.rem(c + 8 - i, 8)], crecv.at[i - 1], (r, c))
        gs_ref[r] = sum(parts[i] for i in range(8))
        for i in range(1, 16):
            push(mine, mine, gsem, grecv, i - 1, (lax.rem(r + i, 16), c))

    def park(step):
        rows = pl.ds(pl.multiple_of(step * UB, UB), UB)
        return (
            pltpu.make_async_copy(whi.at[:, rows, :], spill.at[0, :, rows, :], psem.at[0, step]),
            pltpu.make_async_copy(wlo.at[:, rows, :], spill.at[1, :, rows, :], psem.at[1, step]),
        )

    todo = {j: [] for j in range(STEPS // 2)}
    for j in EVENTS:
        todo[j].append(lambda: next(run))
    for j, f in zip(SECOND_AT, (second_one, second_two, second_three, second_four, second_gram, second_gram_sum)):
        todo[j].append(f)

    def iteration(i, _):
        for j in range(STEPS // 2):
            if todo[j]:
                @pl.when(i == j)
                def _():
                    for f in todo[j]:
                        f()
        for half in range(2):
            step = lax.rem(2 * i + half + STEPS - 1, STEPS)
            slot = lax.rem(step, 16)

            @pl.when((step >= 16) & (2 * i + half >= 1))
            def _():
                for x in park(slot):
                    x.wait()

            rows = pl.ds(pl.multiple_of(slot * UB, UB), UB)
            at = pl.multiple_of((2 * i + half) * UB, UB)
            src, dst = ((wfb, wfa), (wfa, wfb))[half]
            spread_split(at, rows, ins, src, dst, whi, wlo)

            @pl.when(step < 16)
            def _():
                for x in park(slot):
                    x.start()
        return 0

    lax.fori_loop(0, STEPS // 2, iteration, 0)
    for x in park(15):
        x.wait()
    for q in range(128):
        split_rows(q, pl.ds(GRP - UB, UB), wfb, whi, wlo)
    for _ in run:
        pass

    def back(i):
        tiles = pl.ds(pl.multiple_of(i * 32, 32), 32)
        return (
            pltpu.make_async_copy(spill.at[0, tiles], whi.at[tiles], lose.at[0, i]),
            pltpu.make_async_copy(spill.at[1, tiles], wlo.at[tiles], lose.at[1, i]),
        )

    third_gram()
    fold[...] = jnp.zeros((512, 256), F32)
    for first in (True, False):
        def dense(i, _):
            if not first:
                for x in back(i):
                    x.wait()
            y, low = lax.div(i, 2), lax.rem(i, 2)
            tt = jnp.concatenate([t[low + 2 * h, :, :, y].reshape(128, 4096) for h in range(2)], 0)
            side = lambda w: jnp.concatenate([w[i * 32 + j] for j in range(32)], 1)
            lhs = jnp.concatenate([side(whi), side(wlo)], 0)
            res = lax.dot_general(lhs, tt, NT, preferred_element_type=F32)
            fold[pl.ds(GRP if first else 0, GRP), :] += res[:GRP] + res[GRP:]
            if first:
                for x in back(i):
                    x.start()
            return 0

        lax.fori_loop(0, 8, dense, 0)
        if first:
            third_gram_sum()

    one, zero = jnp.ones((), BF), jnp.zeros((), BF)
    second = jnp.zeros((256, 512), F32)
    for j in range(4):
        ij = lax.broadcasted_iota(jnp.int32, (512, 512), 0) + j * 512
        pick = jnp.where(ij == sec_ref[...] - c * 2048, one, zero)
        second += lax.dot_general(s_vm[:, :, :, :, j * 512:(j + 1) * 512].reshape(256, 512), pick, NN, preferred_element_type=F32)
    contrib = second * fold[...].T
    hi = contrib.astype(BF)
    lhs = jnp.concatenate([hi, (contrib - hi.astype(F32)).astype(BF)], 0)
    for j in range(4):
        ii = lax.broadcasted_iota(jnp.int32, (256, 512), 0) + j * 256
        put = jnp.where(ii == own_ref[...] - r * 1024, one, zero)
        res = lax.dot_general(lhs, put, NT, preferred_element_type=F32)
        both = res[:256] + res[256:]
        for h in range(2):
            total[2 * j + h] = both[:, h * 128:(h + 1) * 128]
    for i in range(1, 8):
        to = lax.rem(c + i, 8)
        send_to(total.at[to], got.at[i - 1], rsem.at[i - 1], rrecv.at[i - 1], (r, to))

    for i in range(1, 16):
        take(gs_ref.at[lax.rem(r + 16 - i, 16)], grecv.at[i - 1], (r, c))
        take(gt_ref.at[lax.rem(r + 16 - i, 16)], grecv3.at[i - 1], (r, c))
    invert(gs_ref, gt_ref, a_ref, x_ref, r_ref)
    rows = total[c]
    for i in range(7):
        take(got.at[i], rrecv.at[i], (r, c))
        rows = rows + got[i]
    answer[...] = lax.dot_general(a_ref[...], rows, NN, precision=HIGH, preferred_element_type=F32).reshape(16, 16, 128)

    slot = lax.rem(r, 2) * 8 + c
    lanes = pl.ds(pl.multiple_of(slot * 128, 128), 128)
    for i in range(1, 16):
        to = lax.rem(r + i, 16)
        send_to(answer.at[to], out.at[:, lanes], xsem.at[i], xrecv.at[slot], (to, home))
    here = pltpu.make_async_copy(answer.at[r], out.at[:, lanes], lsem.at[0])
    away = pltpu.make_async_remote_copy(answer.at[r], out.at[:, lanes], xsem.at[0], xrecv.at[slot], device_id=(r, home), device_id_type=MESH)

    @pl.when(at_home)
    def _():
        here.start()

    @pl.when(jnp.logical_not(at_home))
    def _():
        away.start()

    for make, sem, n in sent:
        ref = make()
        pltpu.make_async_remote_copy(ref, ref, sem.at[n], sem.at[n], device_id=(r, c), device_id_type=MESH).wait_send()
    for i in range(1, 8):
        pltpu.make_async_remote_copy(got.at[i - 1], got.at[i - 1], rsem.at[i - 1], rrecv.at[i - 1], device_id=(r, c), device_id_type=MESH).wait_send()
    for i in range(16):
        there = out.at[:, pl.ds(i * 128, 128)]

        @pl.when(jnp.logical_not(at_home & (slot == i)))
        def _():
            take(there, xrecv.at[i], (r, c))

    @pl.when(at_home)
    def _():
        here.wait()

    @pl.when(jnp.logical_not(at_home))
    def _():
        away.wait_send()

    for i in range(1, 16):
        pltpu.make_async_remote_copy(answer.at[0], answer.at[0], xsem.at[i], xrecv.at[0], device_id=(r, c), device_id_type=MESH).wait_send()


def invert(gs_ref, gt_ref, a_ref, x_ref, r_ref):
    gram = (gs_ref[...].reshape(256, 256) / 16384) * (gt_ref[...].reshape(256, 256) / 32768)
    eye = (lax.broadcasted_iota(jnp.int32, (256, 256), 0) == lax.broadcasted_iota(jnp.int32, (256, 256), 1)).astype(F32)
    diag = gram * eye
    down = 1 / jnp.sqrt(jnp.sum(diag, axis=1, keepdims=True))
    along = 1 / jnp.sqrt(jnp.sum(diag, axis=0, keepdims=True))
    a = gram * down * along
    a_ref[...] = a
    bound = jnp.max(jnp.sum(jnp.abs(a), axis=0, keepdims=True), axis=1, keepdims=True)
    scale = 2 / (1 + bound)
    x_ref[...] = eye * scale
    r_ref[...] = eye - a * scale

    def halves(w):
        hi = w.astype(BF)
        return hi, (w - hi.astype(F32)).astype(BF)

    def double(i, _):
        x, rest = x_ref[...], r_ref[...]
        xh, xl = halves(x)
        rh, rl = halves(rest)
        one = lax.dot_general(jnp.concatenate([rh, xh, rl, xl], 0), rh, NN, preferred_element_type=F32)
        two = lax.dot_general(jnp.concatenate([rh, xh], 0), rl, NN, preferred_element_type=F32)
        r_ref[...] = one[:256] + (one[512:768] + two[:256])
        x_ref[...] = x + (one[256:512] + (one[768:] + two[256:]))
        return 0

    lax.fori_loop(0, DOUBLINGS, double, 0)

    def dot(u, w):
        return lax.dot_general(u, w, NN, precision=HIGH, preferred_element_type=F32)

    def newton(i, _):
        now = x_ref[...]
        x_ref[...] = now + dot(now, eye - dot(a_ref[...], now))
        return 0

    lax.fori_loop(0, 3, newton, 0)
    a_ref[...] = x_ref[...] * down * along


DOUBLINGS = 20
EVENTS = (1, 3, 5, 7, 9, 11, 13, 15)
SECOND_AT = (1, 3, 5, 8, 10, 14)


def main(piece, spiece, third, values, length, live, sec, own):
    D = pltpu.SemaphoreType.DMA
    smem = pl.BlockSpec(memory_space=pltpu.SMEM)
    return pl.pallas_call(
        main_body,
        out_shape=(jax.ShapeDtypeStruct((16, 2048), F32), jax.ShapeDtypeStruct((2, 256, GRP, 128), BF)),
        in_specs=[ANY, ANY, INV, INV, smem, smem, INV, INV],
        out_specs=(INV, ANY),
        scratch_shapes=[
            VMEM((4, 4, 2, 4, 16, 4096), BF), VMEM((2, 4, 2, 16, 2048), BF), VMEM((2, 16, 2048), BF), VMEM((2, 16, 2048), BF),
            VMEM((16, 256), F32), VMEM((8, 16, 256), F32),
            VMEM((2, UB * PAD, 128), F32), VMEM((2, UB * PAD, 128), F32),
            VMEM((256, GRP, 128), BF), VMEM((256, GRP, 128), BF), VMEM((512, 256), F32), VMEM((512, 128), F32),
            VMEM((16, 16, 256), F32), VMEM((16, 16, 256), F32), VMEM((8, 256, 128), F32), VMEM((7, 256, 128), F32),
            VMEM((256, 256), F32), VMEM((256, 256), F32), VMEM((256, 256), F32), VMEM((16, 256), F32), VMEM((8, 16, 256), F32), VMEM((16, 16, 128), F32),
            D((SEMS,)), D((SEMS,)), D((14,)), D((14,)), D((7,)), D((7,)), D((15,)), D((15,)), D((2, 16)), D((2,)), D((2, 8)),
            D((7,)), D((7,)), D((16,)), D((16,)), D((7,)), D((7,)), D((15,)), D((15,)),
        ],
        compiler_params=pltpu.CompilerParams(has_side_effects=True, vmem_limit_bytes=67043328, collective_id=0),
        name="factor_update",
    )(piece, spiece, third, values, length, live, sec, own)


def per_device(values, length, owner, second, third, live_blocks, second_factor, third_factor):
    out, _ = main(third_factor.T, second_factor.T, third, values, length, live_blocks, second.reshape(1, 512), owner.reshape(1, 512))
    return out.T


def solution(mesh):
    both = P(("rows", "cols"))
    wide = P(("rows", "cols"), None)
    return jax.shard_map(
        per_device,
        mesh=mesh,
        in_specs=(wide, both, both, both, wide, both, P("cols", "rows"), P("cols", "rows")),
        out_specs=P("cols", "rows"),
        check_vma=False,
    )
```

```python
import jax
import jax.numpy as jnp
from jax import lax
from jax.experimental import pallas as pl
from jax.experimental.pallas import tpu as pltpu
from jax.sharding import PartitionSpec as P

F32 = jnp.float32
BF = jnp.bfloat16
MESH = pl.DeviceIdType.MESH
NT = (((1,), (1,)), ((), ()))
NN = (((1,), (0,)), ((), ()))
HIGH = lax.Precision.HIGHEST
VMEM = pltpu.VMEM
ANY = pl.BlockSpec(memory_space=pl.ANY)
INV = pl.BlockSpec(memory_space=pltpu.VMEM)

PARTS = ((0, 1152), (1152, 1408), (2560, 1536))
ORDERS = ("xyz", "yzx", "zxy")
SENDS = 12
SEMS = 75


def place():
    r, c = lax.axis_index("rows"), lax.axis_index("cols")
    return {"z": lax.div(r, 8) * 2 + lax.rem(c, 2), "x": lax.rem(lax.div(r, 2), 4), "k": lax.rem(r, 2), "y": lax.div(c, 2)}


def device(at):
    return (lax.div(at["z"], 2) * 8 + at["x"] * 2 + at["k"], at["y"] * 2 + lax.rem(at["z"], 2))


class Gather:
    def __init__(self, t, send, recv):
        self.t, self.send, self.recv = t, send, recv
        self.me = me = place()
        self.mine = device(me)
        self.steps = {d: [me[d], *(lax.rem(me[d] + i, 4) for i in (1, 2, 3))] for d in "zxy"}
        self.other = {**me, "k": 1 - me["k"]}
        self.used = 0

    def moved(self, at, dim, step):
        return {**at, dim: self.steps[dim][step]}

    def block(self, part, at, half=None):
        start, size = PARTS[part]
        if half is not None:
            first = (size // 128 // 2) * 128
            start, size = (start, first) if half == 0 else (start + first, size - first)
        return self.t.at[at["z"], at["x"], at["k"], at["y"], :, pl.ds(start, size)]

    def set_of(self, part, at, whole):
        start, size = PARTS[part]
        return self.t.at[*[slice(None) if d in whole else at[d] for d in "zxky"], :, pl.ds(start, size)]

    def new(self):
        self.used += 1
        return self.used - 1

    def copy(self, ref, n, to, group):
        c = pltpu.make_async_remote_copy(ref, ref, self.send.at[group], self.recv.at[n], device_id=device(to), device_id_type=MESH)
        c.start()

    def arrived(self, ref, n):
        pltpu.make_async_remote_copy(ref, ref, self.send.at[0], self.recv.at[n], device_id=self.mine, device_id_type=MESH).wait_recv()

    def run(self):
        me = self.me
        FORE, BACK = 1, 3
        parts = range(3)
        one = {(p, s): self.new() for p in parts for s in (FORE, BACK)}
        onef = {p: self.new() for p in parts}
        two = {(p, o, s): self.new() for p in parts for o in range(4) for s in (FORE, BACK)}
        twof = {p: self.new() for p in parts}
        three = {(p, b, s): self.new() for p in parts for b in range(4) for s in (FORE, BACK)}
        threef = {(p, o): self.new() for p in parts for o in range(4)}
        core = {p: self.new() for p in parts}

        def dims(p):
            return ORDERS[p]

        def at1(p, a):
            return self.moved(me, dims(p)[0], a)

        def at2(p, a, b):
            return self.moved(at1(p, a), dims(p)[1], b)

        def set3(p, b, c, k=None):
            d = dims(p)
            at = self.moved(self.moved(me, d[1], b), d[2], c)
            if k is not None:
                at = {**at, "k": k}
            return self.set_of(p, at, d[0])

        def to(p, i, s):
            return self.moved(me, dims(p)[i], s)

        def cross(p, b, c):
            self.copy(set3(p, b, c), core[p], self.other, p)

        def third(p, a, b):
            for s3 in (FORE, BACK):
                self.copy(self.block(p, at2(p, a, b)), three[p, b, s3], to(p, 2, s3), p)

        for p in parts:
            for s in (FORE, BACK):
                self.copy(self.block(p, me), one[p, s], to(p, 0, s), 6 + p)
        for p in parts:
            for s in (FORE, BACK):
                self.copy(self.block(p, me), two[p, 0, s], to(p, 1, s), 3 + p)
        for p in parts:
            third(p, 0, 0)
        yield
        for p in parts:
            for s in (FORE, BACK):
                back = 4 - s
                self.arrived(self.block(p, at1(p, back)), one[p, s])
                self.copy(self.block(p, at1(p, back), half=0 if s == FORE else 1), onef[p], to(p, 0, s), 9 + p)
                for s2 in (FORE, BACK):
                    self.copy(self.block(p, at1(p, back)), two[p, back, s2], to(p, 1, s2), 3 + p)
                third(p, back, 0)
        yield
        for p in parts:
            self.arrived(self.block(p, at1(p, 2)), onef[p])
            for s2 in (FORE, BACK):
                self.copy(self.block(p, at1(p, 2)), two[p, 2, s2], to(p, 1, s2), 3 + p)
            third(p, 2, 0)
            cross(p, 0, 0)
        yield
        FIRST = {FORE: (0, 3), BACK: (1, 2)}
        for o in (0, 3, 1, 2):
            for p in parts:
                for s in (FORE, BACK):
                    back = 4 - s
                    self.arrived(self.block(p, at2(p, o, back)), two[p, o, s])
                    if o in FIRST[s]:
                        self.copy(self.block(p, at2(p, o, back)), twof[p], to(p, 1, s), 6 + p)
                    third(p, o, back)
        for p in parts:
            for b in (3, 1):
                cross(p, b, 0)
        yield
        for p in parts:
            self.arrived(set3(p, 2, 0), twof[p])
            for o in (0, 3, 1, 2):
                third(p, o, 2)
            cross(p, 2, 0)
        for b in (0, 3, 1, 2):
            yield
            for p in parts:
                for s in (FORE, BACK):
                    back = 4 - s
                    self.arrived(set3(p, b, back), three[p, b, s])
                    if b in FIRST[s]:
                        self.copy(set3(p, b, back), threef[p, b], to(p, 2, s), 3 + p)
                    cross(p, b, back)
        yield
        for b in (0, 3, 1, 2):
            for p in parts:
                self.arrived(set3(p, b, 2), threef[p, b])
                cross(p, b, 2)
        for p in parts:
            start, size = PARTS[p]
            lanes = pl.ds(start, size)
            t = self.t
            self.arrived(t.at[:, :, self.other["k"], :, :, lanes], core[p])
            for n, ref in (
                (p, t.at[0:3, :, :, :, :, lanes]),
                (3 + p, t.at[0, 0:3, :, :, :, lanes]),
                (6 + p, t.at[0, 0, :, 0:3, :, lanes]),
                (9 + p, t.at[0, 0, 0, 0, :, lanes]),
            ):
                pltpu.make_async_remote_copy(ref, ref, self.send.at[n], self.recv.at[0], device_id=self.mine, device_id_type=MESH).wait_send()


UB = 16
STEPS = 512 // UB
GRP = 256
PAD = 129


def spread_pair(at, pair, ins, dst):
    third_ref, value_ref, length_ref, live_ref = ins
    lane = lax.broadcasted_iota(jnp.int32, (16, 128), 1)
    iq = lax.broadcasted_iota(jnp.int32, (128, 128), 0).astype(F32).astype(BF)
    ip = lax.broadcasted_iota(jnp.int32, (256, 128), 0).astype(F32).astype(BF)
    zero = jnp.zeros((128, 128), BF)

    def wide(one, n):
        return jnp.concatenate([one] * (n // 16), axis=0)

    qs, ps = [], []
    for j in range(2):
        b = at + 2 * pair + j
        third = jnp.broadcast_to(third_ref[pl.ds(b, 1), :], (16, 128))
        value = jnp.broadcast_to(value_ref[pl.ds(b, 1), :], (16, 128))
        used = jnp.where(b < live_ref[0], length_ref[b], 0)
        value = wide(jnp.where(lane < used, value, 0.0).astype(BF), 128)
        high = wide((third >> 8).astype(F32).astype(BF), 128)
        low = wide((third & 255).astype(F32).astype(BF), 256)
        qs.append(jnp.where(iq == high, value, zero))
        ps.append(jnp.where(ip == low, jnp.ones((), BF), jnp.zeros((), BF)))
    lhs = jnp.concatenate([jnp.concatenate([qs[0], zero], 1), jnp.concatenate([zero, qs[1]], 1)], 0)
    w = lax.dot_general(lhs, jnp.concatenate(ps, 1), NT, preferred_element_type=F32)
    for j in range(2):
        for h in range(2):
            dst[h, pl.ds((2 * pair + j) * PAD, 128), :] = w[j * 128:(j + 1) * 128, h * 128:(h + 1) * 128]


def split_rows(q, rows, src, whi, wlo):
    for h in range(2):
        f = src[h, pl.ds(q, UB, stride=PAD), :]
        hi = f.astype(BF)
        whi[q * 2 + h, rows, :] = hi
        wlo[q * 2 + h, rows, :] = (f - hi.astype(F32)).astype(BF)


def spread_split(at, rows, ins, src, dst, whi, wlo):
    for pair in range(UB // 2):
        spread_pair(at, pair, ins, dst)
        for q in range(pair * 16, pair * 16 + 16):
            split_rows(q, rows, src, whi, wlo)


def send_to(src, dst, ssem, rsem, to):
    c = pltpu.make_async_remote_copy(src, dst, ssem, rsem, device_id=to, device_id_type=MESH)
    c.start()
    return c


def take(ref, sem, me):
    pltpu.make_async_remote_copy(ref, ref, sem, sem, device_id=me, device_id_type=MESH).wait_recv()


def main_body(piece, spiece, third_ref, values_ref, length_ref, live_ref, sec_ref, own_ref, out, spill,
              t, s_vm, near, far, part, parts, wfa, wfb, whi, wlo, fold, picked, value_ref, gt_ref, gs_ref, total, got, a_ref, x_ref, r_ref, part3, parts3, answer,
              send, recv, ssem, srecv, csem, crecv, gsem, grecv, psem, lsem, lose, rsem, rrecv, xsem, xrecv, csem3, crecv3, gsem3, grecv3):
    r, c = lax.axis_index("rows"), lax.axis_index("cols")
    g = Gather(t, send, recv)
    me = g.me
    cp = pltpu.make_async_copy(piece, t.at[me["z"], me["x"], me["k"], me["y"]], lsem.at[0])
    cp.start()
    cs = pltpu.make_async_copy(spiece, s_vm.at[lax.div(me["z"], 2), me["x"], me["k"]], lsem.at[1])
    cs.start()
    peers = [(lax.rem(r + i, 16), c) for i in range(1, 16)] + [(r, lax.rem(c + i, 8)) for i in range(1, 8)]
    peers += [device(g.moved(me, "z", 1)), device(g.moved(me, "z", 3))]
    barrier = pltpu.get_barrier_semaphore()
    for to in peers:
        pl.semaphore_signal(barrier, inc=1, device_id=to, device_id_type=MESH)
    home = lax.div(r, 2)
    at_home = home == c
    for i in range(16):
        source = (2 * c + i // 8, i % 8)

        @pl.when(jnp.logical_not((source[0] == r) & (c == source[1])))
        def _():
            pl.semaphore_signal(barrier, inc=1, device_id=source, device_id_type=MESH)
    value_ref[...] = values_ref[...].astype(F32)
    ins = (third_ref, value_ref, length_ref, live_ref)
    pl.semaphore_wait(barrier, 40 - at_home.astype(jnp.int32))
    sent = []

    def push(src, dst, ssem, rsem, to):
        send_to(src, dst, ssem, rsem, to)

    cp.wait()
    run = g.run()
    next(run)
    cs.wait()
    FORE, BACK = 1, 3
    relay = {FORE: near, BACK: far}

    def hop(src, dst, n, to):
        send_to(src(), dst(), ssem.at[n], srecv.at[n], device(to))
        sent.append((src, ssem, n))

    xs = g.steps["x"]
    zs = [lax.div(z, 2) for z in g.steps["z"]]

    def plane(z, x=None, half=None):
        ref = s_vm.at[zs[z], slice(None) if x is None else xs[x], me["k"]]
        return ref if half is None else ref.at[:, pl.ds(half * 1024, 1024)]

    def stop(way, j):
        return relay[way].at[j]

    for n, way in enumerate((FORE, BACK)):
        hop(lambda: plane(0, 0), lambda: plane(0, 0), n, g.moved(me, "x", way))

    def second_one():
        for n, way in enumerate((FORE, BACK)):
            take(plane(0, 4 - way), srecv.at[n], (r, c))
            half = lambda n=n, way=way: plane(0, 4 - way, half=n)
            hop(half, half, 2 + n, g.moved(me, "x", way))

    def second_two():
        for n, way in enumerate((FORE, BACK)):
            take(plane(0, 2, half=n), srecv.at[2 + n], (r, c))
        for n, way in enumerate((FORE, BACK)):
            for j in range(2):
                hop(lambda n=n, j=j: plane(0, 2 * n + j), lambda: stop(way, j), 4 + 2 * n + j, g.moved(me, "z", way))
        hop(lambda: plane(0), lambda: plane(0), 12, g.other)

    def second_three():
        for n, way in enumerate((FORE, BACK)):
            for j in range(2):
                take(stop(way, j), srecv.at[4 + 2 * n + j], (r, c))
                hop(lambda way=way, j=j: stop(way, j), lambda: plane(4 - way, 2 * n + j), 8 + 2 * n + j, g.moved(me, "z", way))

    def second_four():
        for n in range(2):
            for j in range(2):
                take(plane(2, 2 * n + j), srecv.at[8 + 2 * n + j], (r, c))
        hop(lambda: plane(2), lambda: plane(2), 13, g.other)

    mine = gs_ref.at[r]

    mine3 = gt_ref.at[r]

    def third_gram():
        y, low = me["y"], lax.rem(me["z"], 2)
        whole = jnp.concatenate([t[low + 2 * h, :, :, y].reshape(128, 4096) for h in range(2)], 0)
        chunk = lax.dot_general(t[me["z"], me["x"], me["k"], y], whole, NT, preferred_element_type=F32)
        part3[...] = chunk
        parts3[c] = chunk
        for i in range(1, 8):
            push(part3, parts3.at[c], csem3, crecv3, (r, lax.rem(c + i, 8)))

    def third_gram_sum():
        take(parts3.at[0:7], crecv3, (r, c))
        gt_ref[r] = sum(parts3[i] for i in range(8))
        for i in range(1, 16):
            push(mine3, mine3, gsem3, grecv3, (lax.rem(r + i, 16), c))

    def second_gram():
        for n, z in ((12, 0), (13, 2)):
            take(s_vm.at[zs[z], :, g.other["k"]], srecv.at[n], (r, c))
        chunk = lax.dot_general(s_vm[zs[0], me["x"], me["k"]], s_vm[...].reshape(256, 2048), NT, preferred_element_type=F32)
        part[...] = chunk
        parts[c] = chunk
        for i in range(1, 8):
            push(part, parts.at[c], csem, crecv, (r, lax.rem(c + i, 8)))

    def second_gram_sum():
        take(parts.at[0:7], crecv, (r, c))
        gs_ref[r] = sum(parts[i] for i in range(8))
        for i in range(1, 16):
            push(mine, mine, gsem, grecv, (lax.rem(r + i, 16), c))

    def parked(step):
        both = spill.at[:, :, pl.ds(pl.multiple_of(step * UB, UB), UB), :]
        pltpu.make_async_copy(both, both, psem.at[step]).wait()

    def park(step):
        rows = pl.ds(pl.multiple_of(step * UB, UB), UB)
        return (
            pltpu.make_async_copy(whi.at[:, rows, :], spill.at[0, :, rows, :], psem.at[step]),
            pltpu.make_async_copy(wlo.at[:, rows, :], spill.at[1, :, rows, :], psem.at[step]),
        )

    todo = {j: [] for j in range(STEPS // 2)}
    for j in EVENTS:
        todo[j].append(lambda: next(run))
    for j, f in zip(SECOND_AT, (second_one, second_two, second_three, second_four)):
        todo[j].append(f)

    def iteration(i, _):
        for j in range(STEPS // 2):
            if todo[j]:
                @pl.when(i == j)
                def _():
                    for f in todo[j]:
                        f()
        for half in range(2):
            step = lax.rem(2 * i + half + STEPS - 1, STEPS)
            slot = lax.rem(step, 16)

            @pl.when((step >= 16) & (2 * i + half >= 1))
            def _():
                parked(slot)

            rows = pl.ds(pl.multiple_of(slot * UB, UB), UB)
            at = pl.multiple_of((2 * i + half) * UB, UB)
            src, dst = ((wfb, wfa), (wfa, wfb))[half]
            spread_split(at, rows, ins, src, dst, whi, wlo)

            @pl.when(step < 16)
            def _():
                for x in park(slot):
                    x.start()
        return 0

    lax.fori_loop(0, STEPS // 2, iteration, 0)
    parked(15)
    for q in range(128):
        split_rows(q, pl.ds(GRP - UB, UB), wfb, whi, wlo)
    second_gram()
    one, zero = jnp.ones((), BF), jnp.zeros((), BF)
    second = jnp.zeros((256, 512), F32)
    for j in range(4):
        ij = lax.broadcasted_iota(jnp.int32, (512, 512), 0) + j * 512
        pick = jnp.where(ij == sec_ref[...] - c * 2048, one, zero)
        second += lax.dot_general(s_vm[:, :, :, :, j * 512:(j + 1) * 512].reshape(256, 512), pick, NN, preferred_element_type=F32)
    picked[...] = second
    for _ in run:
        pass

    def back(i):
        tiles = pl.ds(pl.multiple_of(i * 64, 64), 64)
        return (
            pltpu.make_async_copy(spill.at[0, tiles], whi.at[tiles], lose.at[i]),
            pltpu.make_async_copy(spill.at[1, tiles], wlo.at[tiles], lose.at[i]),
        )

    third_gram()
    fold[...] = jnp.zeros((512, 256), F32)
    for first in (True, False):
        def dense(i, _):
            if not first:
                both = spill.at[:, pl.ds(pl.multiple_of(i * 64, 64), 64)]
                pltpu.make_async_copy(both, both, lose.at[i]).wait()
            tt = jnp.concatenate(
                [jnp.concatenate([t[low + 2 * h, :, :, i].reshape(128, 4096) for h in range(2)], 0) for low in range(2)], 1
            )
            side = lambda w: jnp.concatenate([w[i * 64 + j] for j in range(64)], 1)
            lhs = jnp.concatenate([side(whi), side(wlo)], 0)
            res = lax.dot_general(lhs, tt, NT, preferred_element_type=F32)
            fold[pl.ds(GRP if first else 0, GRP), :] += res[:GRP] + res[GRP:]
            if first:
                for x in back(i):
                    x.start()
            return 0

        lax.fori_loop(0, 4, dense, 0)
        if first:
            second_gram_sum()
            third_gram_sum()

    contrib = picked[...] * fold[...].T
    hi = contrib.astype(BF)
    lhs = jnp.concatenate([hi, (contrib - hi.astype(F32)).astype(BF)], 0)
    for j in range(4):
        ii = lax.broadcasted_iota(jnp.int32, (256, 512), 0) + j * 256
        put = jnp.where(ii == own_ref[...] - r * 1024, one, zero)
        res = lax.dot_general(lhs, put, NT, preferred_element_type=F32)
        both = res[:256] + res[256:]
        for h in range(2):
            total[2 * j + h] = both[:, h * 128:(h + 1) * 128]
    for i in range(1, 8):
        to = lax.rem(c + i, 8)
        send_to(total.at[to], got.at[i - 1], rsem, rrecv, (r, to))

    take(gs_ref.at[0:15], grecv, (r, c))
    take(gt_ref.at[0:15], grecv3, (r, c))
    invert(gs_ref, gt_ref, a_ref, x_ref, r_ref)
    rows = total[c]
    take(got, rrecv, (r, c))
    for i in range(7):
        rows = rows + got[i]
    answer[...] = lax.dot_general(a_ref[...], rows, NN, precision=HIGH, preferred_element_type=F32).reshape(16, 16, 128)

    slot = lax.rem(r, 2) * 8 + c
    lanes = pl.ds(pl.multiple_of(slot * 128, 128), 128)
    for i in range(1, 16):
        to = lax.rem(r + i, 16)
        send_to(answer.at[to], out.at[:, lanes], xsem, xrecv, (to, home))
    here = pltpu.make_async_copy(answer.at[r], out.at[:, lanes], lsem.at[0])
    away = pltpu.make_async_remote_copy(answer.at[r], out.at[:, lanes], xsem, xrecv, device_id=(r, home), device_id_type=MESH)

    @pl.when(at_home)
    def _():
        here.start()

    @pl.when(jnp.logical_not(at_home))
    def _():
        away.start()

    for make, sem, n in sent:
        ref = make()
        pltpu.make_async_remote_copy(ref, ref, sem.at[n], sem.at[n], device_id=(r, c), device_id_type=MESH).wait_send()
    def all_sent(ref, sem):
        pltpu.make_async_remote_copy(ref, ref, sem, sem, device_id=(r, c), device_id_type=MESH).wait_send()

    all_sent(got, rsem)
    all_sent(parts.at[0:7], csem)
    all_sent(parts3.at[0:7], csem3)
    all_sent(gs_ref.at[0:15], gsem)
    all_sent(gt_ref.at[0:15], gsem3)

    @pl.when(at_home)
    def _():
        take(out.at[:, 0:1920], xrecv, (r, c))
        here.wait()
        all_sent(answer.at[0:15], xsem)

    @pl.when(jnp.logical_not(at_home))
    def _():
        take(out, xrecv, (r, c))
        all_sent(answer, xsem)


def invert(gs_ref, gt_ref, a_ref, x_ref, r_ref):
    gram = (gs_ref[...].reshape(256, 256) / 16384) * (gt_ref[...].reshape(256, 256) / 32768)
    eye = (lax.broadcasted_iota(jnp.int32, (256, 256), 0) == lax.broadcasted_iota(jnp.int32, (256, 256), 1)).astype(F32)
    diag = gram * eye
    down = 1 / jnp.sqrt(jnp.sum(diag, axis=1, keepdims=True))
    along = 1 / jnp.sqrt(jnp.sum(diag, axis=0, keepdims=True))
    a = gram * down * along
    a_ref[...] = a
    bound = jnp.max(jnp.sum(jnp.abs(a), axis=0, keepdims=True), axis=1, keepdims=True)
    scale = 2 / (1 + bound)
    x_ref[...] = eye * scale
    r_ref[...] = eye - a * scale

    def halves(w):
        hi = w.astype(BF)
        return hi, (w - hi.astype(F32)).astype(BF)

    def double(i, _):
        x, rest = x_ref[...], r_ref[...]
        xh, xl = halves(x)
        rh, rl = halves(rest)
        one = lax.dot_general(jnp.concatenate([rh, xh, rl, xl], 0), rh, NN, preferred_element_type=F32)
        two = lax.dot_general(jnp.concatenate([rh, xh], 0), rl, NN, preferred_element_type=F32)
        r_ref[...] = one[:256] + (one[512:768] + two[:256])
        x_ref[...] = x + (one[256:512] + (one[768:] + two[256:]))
        return 0

    lax.fori_loop(0, DOUBLINGS, double, 0)

    def dot(u, w):
        return lax.dot_general(u, w, NN, precision=HIGH, preferred_element_type=F32)

    def newton(i, _):
        now = x_ref[...]
        x_ref[...] = now + dot(now, eye - dot(a_ref[...], now))
        return 0

    lax.fori_loop(0, 3, newton, 0)
    a_ref[...] = x_ref[...] * down * along


DOUBLINGS = 20
EVENTS = (1, 3, 5, 7, 9, 11, 13, 15)
SECOND_AT = (1, 3, 10, 15)


def main(piece, spiece, third, values, length, live, sec, own):
    D = pltpu.SemaphoreType.DMA
    smem = pl.BlockSpec(memory_space=pltpu.SMEM)
    return pl.pallas_call(
        main_body,
        out_shape=(jax.ShapeDtypeStruct((16, 2048), F32), jax.ShapeDtypeStruct((2, 256, GRP, 128), BF)),
        in_specs=[ANY, ANY, INV, INV, smem, smem, INV, INV],
        out_specs=(INV, ANY),
        scratch_shapes=[
            VMEM((4, 4, 2, 4, 16, 4096), BF), VMEM((2, 4, 2, 16, 2048), BF), VMEM((2, 16, 2048), BF), VMEM((2, 16, 2048), BF),
            VMEM((16, 256), F32), VMEM((8, 16, 256), F32),
            VMEM((2, UB * PAD, 128), F32), VMEM((2, UB * PAD, 128), F32),
            VMEM((256, GRP, 128), BF), VMEM((256, GRP, 128), BF), VMEM((512, 256), F32), VMEM((256, 512), F32), VMEM((512, 128), F32),
            VMEM((16, 16, 256), F32), VMEM((16, 16, 256), F32), VMEM((8, 256, 128), F32), VMEM((7, 256, 128), F32),
            VMEM((256, 256), F32), VMEM((256, 256), F32), VMEM((256, 256), F32), VMEM((16, 256), F32), VMEM((8, 16, 256), F32), VMEM((16, 16, 128), F32),
            D((SENDS,)), D((SEMS,)), D((14,)), D((14,)), *[D(())] * 4, D((16,)), D((2,)), D((4,)), *[D(())] * 8,
        ],
        compiler_params=pltpu.CompilerParams(has_side_effects=True, vmem_limit_bytes=67043328, collective_id=0),
        name="factor_update",
    )(piece, spiece, third, values, length, live, sec, own)


def per_device(values, length, owner, second, third, live_blocks, second_factor, third_factor):
    out, _ = main(third_factor.T, second_factor.T, third, values, length, live_blocks, second.reshape(1, 512), owner.reshape(1, 512))
    return out.T


def solution(mesh):
    both = P(("rows", "cols"))
    wide = P(("rows", "cols"), None)
    return jax.shard_map(
        per_device,
        mesh=mesh,
        in_specs=(wide, both, both, both, wide, both, P("cols", "rows"), P("cols", "rows")),
        out_specs=P("cols", "rows"),
        check_vma=False,
    )
```

```python
import jax
import jax.numpy as jnp
from jax import lax
from jax.experimental import pallas as pl
from jax.experimental.pallas import tpu as pltpu
from jax.sharding import PartitionSpec as P

F32 = jnp.float32
BF = jnp.bfloat16
MESH = pl.DeviceIdType.MESH
NT = (((1,), (1,)), ((), ()))
NN = (((1,), (0,)), ((), ()))
HIGH = lax.Precision.HIGHEST
VMEM = pltpu.VMEM
ANY = pl.BlockSpec(memory_space=pl.ANY)
INV = pl.BlockSpec(memory_space=pltpu.VMEM)

PARTS = ((0, 1152), (1152, 1408), (2560, 1536))
ORDERS = ("xyz", "yzx", "zxy")
SENDS = 12
SEMS = 75


def place():
    r, c = lax.axis_index("rows"), lax.axis_index("cols")
    return {"z": lax.div(r, 8) * 2 + lax.rem(c, 2), "x": lax.rem(lax.div(r, 2), 4), "k": lax.rem(r, 2), "y": lax.div(c, 2)}


def device(at):
    return (lax.div(at["z"], 2) * 8 + at["x"] * 2 + at["k"], at["y"] * 2 + lax.rem(at["z"], 2))


class Gather:
    def __init__(self, t, send, recv):
        self.t, self.send, self.recv = t, send, recv
        self.me = me = place()
        self.mine = device(me)
        self.steps = {d: [me[d], *(lax.rem(me[d] + i, 4) for i in (1, 2, 3))] for d in "zxy"}
        self.other = {**me, "k": 1 - me["k"]}
        self.used = 0

    def moved(self, at, dim, step):
        return {**at, dim: self.steps[dim][step]}

    def block(self, part, at, half=None):
        start, size = PARTS[part]
        if half is not None:
            first = (size // 128 // 2) * 128
            start, size = (start, first) if half == 0 else (start + first, size - first)
        return self.t.at[at["z"], at["x"], at["k"], at["y"], :, pl.ds(start, size)]

    def set_of(self, part, at, whole):
        start, size = PARTS[part]
        return self.t.at[*[slice(None) if d in whole else at[d] for d in "zxky"], :, pl.ds(start, size)]

    def new(self):
        self.used += 1
        return self.used - 1

    def copy(self, ref, n, to, group):
        c = pltpu.make_async_remote_copy(ref, ref, self.send.at[group], self.recv.at[n], device_id=device(to), device_id_type=MESH)
        c.start()

    def arrived(self, ref, n):
        pltpu.make_async_remote_copy(ref, ref, self.send.at[0], self.recv.at[n], device_id=self.mine, device_id_type=MESH).wait_recv()

    def run(self):
        me = self.me
        FORE, BACK = 1, 3
        parts = range(3)
        one = {(p, s): self.new() for p in parts for s in (FORE, BACK)}
        onef = {p: self.new() for p in parts}
        two = {(p, o, s): self.new() for p in parts for o in range(4) for s in (FORE, BACK)}
        twof = {p: self.new() for p in parts}
        three = {(p, b, s): self.new() for p in parts for b in range(4) for s in (FORE, BACK)}
        threef = {(p, o): self.new() for p in parts for o in range(4)}
        core = {p: self.new() for p in parts}

        def dims(p):
            return ORDERS[p]

        def at1(p, a):
            return self.moved(me, dims(p)[0], a)

        def at2(p, a, b):
            return self.moved(at1(p, a), dims(p)[1], b)

        def set3(p, b, c, k=None):
            d = dims(p)
            at = self.moved(self.moved(me, d[1], b), d[2], c)
            if k is not None:
                at = {**at, "k": k}
            return self.set_of(p, at, d[0])

        def to(p, i, s):
            return self.moved(me, dims(p)[i], s)

        def cross(p, b, c):
            self.copy(set3(p, b, c), core[p], self.other, p)

        def third(p, a, b):
            for s3 in (FORE, BACK):
                self.copy(self.block(p, at2(p, a, b)), three[p, b, s3], to(p, 2, s3), p)

        for p in parts:
            for s in (FORE, BACK):
                self.copy(self.block(p, me), one[p, s], to(p, 0, s), 6 + p)
        for p in parts:
            for s in (FORE, BACK):
                self.copy(self.block(p, me), two[p, 0, s], to(p, 1, s), 3 + p)
        for p in parts:
            third(p, 0, 0)
        yield
        for p in parts:
            for s in (FORE, BACK):
                back = 4 - s
                self.arrived(self.block(p, at1(p, back)), one[p, s])
                self.copy(self.block(p, at1(p, back), half=0 if s == FORE else 1), onef[p], to(p, 0, s), 9 + p)
                for s2 in (FORE, BACK):
                    self.copy(self.block(p, at1(p, back)), two[p, back, s2], to(p, 1, s2), 3 + p)
                third(p, back, 0)
        yield
        for p in parts:
            self.arrived(self.block(p, at1(p, 2)), onef[p])
            for s2 in (FORE, BACK):
                self.copy(self.block(p, at1(p, 2)), two[p, 2, s2], to(p, 1, s2), 3 + p)
            third(p, 2, 0)
            cross(p, 0, 0)
        yield
        FIRST = {FORE: (0, 3), BACK: (1, 2)}
        for o in (0, 3, 1, 2):
            for p in parts:
                for s in (FORE, BACK):
                    back = 4 - s
                    self.arrived(self.block(p, at2(p, o, back)), two[p, o, s])
                    if o in FIRST[s]:
                        self.copy(self.block(p, at2(p, o, back)), twof[p], to(p, 1, s), 6 + p)
                    third(p, o, back)
        for p in parts:
            for b in (3, 1):
                cross(p, b, 0)
        yield
        for p in parts:
            self.arrived(set3(p, 2, 0), twof[p])
            for o in (0, 3, 1, 2):
                third(p, o, 2)
            cross(p, 2, 0)
        for b in (0, 3, 1, 2):
            yield
            for p in parts:
                for s in (FORE, BACK):
                    back = 4 - s
                    self.arrived(set3(p, b, back), three[p, b, s])
                    if b in FIRST[s]:
                        self.copy(set3(p, b, back), threef[p, b], to(p, 2, s), 3 + p)
                    cross(p, b, back)
        yield
        for b in (0, 3, 1, 2):
            for p in parts:
                self.arrived(set3(p, b, 2), threef[p, b])
                cross(p, b, 2)
        for p in parts:
            start, size = PARTS[p]
            lanes = pl.ds(start, size)
            t = self.t
            self.arrived(t.at[:, :, self.other["k"], :, :, lanes], core[p])
            for n, ref in (
                (p, t.at[0:3, :, :, :, :, lanes]),
                (3 + p, t.at[0, 0:3, :, :, :, lanes]),
                (6 + p, t.at[0, 0, :, 0:3, :, lanes]),
                (9 + p, t.at[0, 0, 0, 0, :, lanes]),
            ):
                pltpu.make_async_remote_copy(ref, ref, self.send.at[n], self.recv.at[0], device_id=self.mine, device_id_type=MESH).wait_send()


UB = 16
STEPS = 512 // UB
GRP = 256
PAD = 129


def spread_pair(at, pair, ins, dst):
    third_ref, value_ref, length_ref, live_ref = ins
    lane = lax.broadcasted_iota(jnp.int32, (16, 128), 1)
    iq = lax.broadcasted_iota(jnp.int32, (128, 128), 0).astype(F32).astype(BF)
    ip = lax.broadcasted_iota(jnp.int32, (256, 128), 0).astype(F32).astype(BF)
    zero = jnp.zeros((128, 128), BF)

    def wide(one, n):
        return jnp.concatenate([one] * (n // 16), axis=0)

    qs, ps = [], []
    for j in range(2):
        b = at + 2 * pair + j
        third = jnp.broadcast_to(third_ref[pl.ds(b, 1), :], (16, 128))
        value = jnp.broadcast_to(value_ref[pl.ds(b, 1), :], (16, 128))
        used = jnp.where(b < live_ref[0], length_ref[b], 0)
        value = wide(jnp.where(lane < used, value, 0.0).astype(BF), 128)
        high = wide((third >> 8).astype(F32).astype(BF), 128)
        low = wide((third & 255).astype(F32).astype(BF), 256)
        qs.append(jnp.where(iq == high, value, zero))
        ps.append(jnp.where(ip == low, jnp.ones((), BF), jnp.zeros((), BF)))
    lhs = jnp.concatenate([jnp.concatenate([qs[0], zero], 1), jnp.concatenate([zero, qs[1]], 1)], 0)
    w = lax.dot_general(lhs, jnp.concatenate(ps, 1), NT, preferred_element_type=F32)
    for j in range(2):
        for h in range(2):
            dst[h, pl.ds((2 * pair + j) * PAD, 128), :] = w[j * 128:(j + 1) * 128, h * 128:(h + 1) * 128]


def split_rows(q, rows, src, whi, wlo):
    for h in range(2):
        f = src[h, pl.ds(q, UB, stride=PAD), :]
        hi = f.astype(BF)
        whi[q * 2 + h, rows, :] = hi
        wlo[q * 2 + h, rows, :] = (f - hi.astype(F32)).astype(BF)


def spread_split(at, rows, ins, src, dst, whi, wlo):
    for pair in range(UB // 2):
        spread_pair(at, pair, ins, dst)
        for q in range(pair * 16, pair * 16 + 16):
            split_rows(q, rows, src, whi, wlo)


def send_to(src, dst, ssem, rsem, to):
    c = pltpu.make_async_remote_copy(src, dst, ssem, rsem, device_id=to, device_id_type=MESH)
    c.start()
    return c


def take(ref, sem, me):
    pltpu.make_async_remote_copy(ref, ref, sem, sem, device_id=me, device_id_type=MESH).wait_recv()


def main_body(piece, spiece, third_ref, values_ref, length_ref, live_hbm, sec_ref, own_ref, out, spill,
              t, s_vm, near, far, part, parts, wfa, wfb, whi, wlo, fold, picked, value_ref, live_ref, gt_ref, gs_ref, total, got, a_ref, x_ref, r_ref, part3, parts3, answer,
              send, recv, ssem, srecv, csem, crecv, gsem, grecv, psem, lsem, lose, rsem, rrecv, xsem, xrecv, csem3, crecv3, gsem3, grecv3):
    r, c = lax.axis_index("rows"), lax.axis_index("cols")
    g = Gather(t, send, recv)
    me = g.me
    cp = pltpu.make_async_copy(piece, t.at[me["z"], me["x"], me["k"], me["y"]], lsem.at[0])
    cp.start()
    cs = pltpu.make_async_copy(spiece, s_vm.at[lax.div(me["z"], 2), me["x"], me["k"]], lsem.at[1])
    cs.start()
    home = lax.div(r, 2)
    at_home = home == c
    barrier = pltpu.get_barrier_semaphore()
    for to in [device(g.moved(me, d, way)) for d in "xyz" for way in (1, 3)] + [device(g.other)]:
        pl.semaphore_signal(barrier, inc=1, device_id=to, device_id_type=MESH)
    cl = pltpu.make_async_copy(live_hbm, live_ref, lsem.at[2])
    cl.start()
    cl.wait()
    value_ref[...] = values_ref[...].astype(F32)
    ins = (third_ref, value_ref, length_ref, live_ref)
    pl.semaphore_wait(barrier, 7)
    sent = []

    def push(src, dst, ssem, rsem, to):
        send_to(src, dst, ssem, rsem, to)

    cp.wait()
    run = g.run()
    next(run)
    cs.wait()
    FORE, BACK = 1, 3
    relay = {FORE: near, BACK: far}

    def hop(src, dst, n, to):
        send_to(src(), dst(), ssem.at[n], srecv.at[n], device(to))
        sent.append((src, ssem, n))

    xs = g.steps["x"]
    zs = [lax.div(z, 2) for z in g.steps["z"]]

    def plane(z, x=None, half=None):
        ref = s_vm.at[zs[z], slice(None) if x is None else xs[x], me["k"]]
        return ref if half is None else ref.at[:, pl.ds(half * 1024, 1024)]

    def stop(way, j):
        return relay[way].at[j]

    for n, way in enumerate((FORE, BACK)):
        hop(lambda: plane(0, 0), lambda: plane(0, 0), n, g.moved(me, "x", way))

    def second_one():
        for n, way in enumerate((FORE, BACK)):
            take(plane(0, 4 - way), srecv.at[n], (r, c))
            half = lambda n=n, way=way: plane(0, 4 - way, half=n)
            hop(half, half, 2 + n, g.moved(me, "x", way))

    def second_two():
        for n, way in enumerate((FORE, BACK)):
            take(plane(0, 2, half=n), srecv.at[2 + n], (r, c))
        for n, way in enumerate((FORE, BACK)):
            for j in range(2):
                hop(lambda n=n, j=j: plane(0, 2 * n + j), lambda: stop(way, j), 4 + 2 * n + j, g.moved(me, "z", way))
        hop(lambda: plane(0), lambda: plane(0), 12, g.other)

    def second_three():
        for n, way in enumerate((FORE, BACK)):
            for j in range(2):
                take(stop(way, j), srecv.at[4 + 2 * n + j], (r, c))
                hop(lambda way=way, j=j: stop(way, j), lambda: plane(4 - way, 2 * n + j), 8 + 2 * n + j, g.moved(me, "z", way))

    def second_four():
        for n in range(2):
            for j in range(2):
                take(plane(2, 2 * n + j), srecv.at[8 + 2 * n + j], (r, c))
        hop(lambda: plane(2), lambda: plane(2), 13, g.other)

    mine = gs_ref.at[r]

    mine3 = gt_ref.at[r]

    def third_gram():
        y, low = me["y"], lax.rem(me["z"], 2)
        whole = jnp.concatenate([t[low + 2 * h, :, :, y].reshape(128, 4096) for h in range(2)], 0)
        chunk = lax.dot_general(t[me["z"], me["x"], me["k"], y], whole, NT, preferred_element_type=F32)
        part3[...] = chunk
        parts3[c] = chunk
        for i in range(1, 8):
            push(part3, parts3.at[c], csem3, crecv3, (r, lax.rem(c + i, 8)))

    def third_gram_sum():
        take(parts3.at[0:7], crecv3, (r, c))
        gt_ref[r] = sum(parts3[i] for i in range(8))
        for i in range(1, 16):
            push(mine3, mine3, gsem3, grecv3, (lax.rem(r + i, 16), c))

    def second_gram():
        for n, z in ((12, 0), (13, 2)):
            take(s_vm.at[zs[z], :, g.other["k"]], srecv.at[n], (r, c))
        chunk = lax.dot_general(s_vm[zs[0], me["x"], me["k"]], s_vm[...].reshape(256, 2048), NT, preferred_element_type=F32)
        part[...] = chunk
        parts[c] = chunk
        for i in range(1, 8):
            push(part, parts.at[c], csem, crecv, (r, lax.rem(c + i, 8)))

    def second_gram_sum():
        take(parts.at[0:7], crecv, (r, c))
        gs_ref[r] = sum(parts[i] for i in range(8))
        for i in range(1, 16):
            push(mine, mine, gsem, grecv, (lax.rem(r + i, 16), c))

    def parked(step):
        both = spill.at[:, :, pl.ds(pl.multiple_of(step * UB, UB), UB), :]
        pltpu.make_async_copy(both, both, psem.at[step]).wait()

    def park(step):
        rows = pl.ds(pl.multiple_of(step * UB, UB), UB)
        return (
            pltpu.make_async_copy(whi.at[:, rows, :], spill.at[0, :, rows, :], psem.at[step]),
            pltpu.make_async_copy(wlo.at[:, rows, :], spill.at[1, :, rows, :], psem.at[step]),
        )

    todo = {j: [] for j in range(STEPS // 2)}
    for j in EVENTS:
        todo[j].append(lambda: next(run))
    for j, f in zip(SECOND_AT, (second_one, second_two, second_three, second_four)):
        todo[j].append(f)

    def iteration(i, _):
        for j in range(STEPS // 2):
            if todo[j]:
                @pl.when(i == j)
                def _():
                    for f in todo[j]:
                        f()
        for half in range(2):
            step = lax.rem(2 * i + half + STEPS - 1, STEPS)
            slot = lax.rem(step, 16)

            @pl.when((step >= 16) & (2 * i + half >= 1))
            def _():
                parked(slot)

            rows = pl.ds(pl.multiple_of(slot * UB, UB), UB)
            at = pl.multiple_of((2 * i + half) * UB, UB)
            src, dst = ((wfb, wfa), (wfa, wfb))[half]
            spread_split(at, rows, ins, src, dst, whi, wlo)

            @pl.when(step < 16)
            def _():
                for x in park(slot):
                    x.start()
        return 0

    lax.fori_loop(0, STEPS // 2, iteration, 0)
    parked(15)
    for q in range(128):
        split_rows(q, pl.ds(GRP - UB, UB), wfb, whi, wlo)
    second_gram()
    one, zero = jnp.ones((), BF), jnp.zeros((), BF)
    second = jnp.zeros((256, 512), F32)
    for j in range(4):
        ij = lax.broadcasted_iota(jnp.int32, (512, 512), 0) + j * 512
        pick = jnp.where(ij == sec_ref[...] - c * 2048, one, zero)
        second += lax.dot_general(s_vm[:, :, :, :, j * 512:(j + 1) * 512].reshape(256, 512), pick, NN, preferred_element_type=F32)
    picked[...] = second
    for _ in run:
        pass

    def back(i):
        tiles = pl.ds(pl.multiple_of(i * 64, 64), 64)
        return (
            pltpu.make_async_copy(spill.at[0, tiles], whi.at[tiles], lose.at[i]),
            pltpu.make_async_copy(spill.at[1, tiles], wlo.at[tiles], lose.at[i]),
        )

    third_gram()
    fold[...] = jnp.zeros((512, 256), F32)
    for first in (True, False):
        def dense(i, _):
            if not first:
                both = spill.at[:, pl.ds(pl.multiple_of(i * 64, 64), 64)]
                pltpu.make_async_copy(both, both, lose.at[i]).wait()
            tt = jnp.concatenate(
                [jnp.concatenate([t[low + 2 * h, :, :, i].reshape(128, 4096) for h in range(2)], 0) for low in range(2)], 1
            )
            side = lambda w: jnp.concatenate([w[i * 64 + j] for j in range(64)], 1)
            lhs = jnp.concatenate([side(whi), side(wlo)], 0)
            res = lax.dot_general(lhs, tt, NT, preferred_element_type=F32)
            fold[pl.ds(GRP if first else 0, GRP), :] += res[:GRP] + res[GRP:]
            if first:
                for x in back(i):
                    x.start()
            return 0

        lax.fori_loop(0, 4, dense, 0)
        if first:
            second_gram_sum()
            third_gram_sum()

    contrib = picked[...] * fold[...].T
    hi = contrib.astype(BF)
    lhs = jnp.concatenate([hi, (contrib - hi.astype(F32)).astype(BF)], 0)
    for j in range(4):
        ii = lax.broadcasted_iota(jnp.int32, (256, 512), 0) + j * 256
        put = jnp.where(ii == own_ref[...] - r * 1024, one, zero)
        res = lax.dot_general(lhs, put, NT, preferred_element_type=F32)
        both = res[:256] + res[256:]
        for h in range(2):
            total[2 * j + h] = both[:, h * 128:(h + 1) * 128]
        for to in (2 * j, 2 * j + 1):
            @pl.when(c != to)
            def _():
                send_to(total.at[to], got.at[lax.rem(to - c + 8, 8) - 1], rsem, rrecv, (r, to))

    take(gs_ref.at[0:15], grecv, (r, c))
    take(gt_ref.at[0:15], grecv3, (r, c))
    invert(gs_ref, gt_ref, a_ref, x_ref, r_ref)
    rows = total[c]
    take(got, rrecv, (r, c))
    for i in range(7):
        rows = rows + got[i]
    answer[...] = lax.dot_general(a_ref[...], rows, NN, precision=HIGH, preferred_element_type=F32).reshape(16, 16, 128)

    slot = lax.rem(r, 2) * 8 + c
    lanes = pl.ds(pl.multiple_of(slot * 128, 128), 128)
    for i in range(1, 16):
        to = lax.rem(r + i, 16)
        send_to(answer.at[to], out.at[:, lanes], xsem, xrecv, (to, home))
    here = pltpu.make_async_copy(answer.at[r], out.at[:, lanes], lsem.at[0])
    away = pltpu.make_async_remote_copy(answer.at[r], out.at[:, lanes], xsem, xrecv, device_id=(r, home), device_id_type=MESH)

    @pl.when(at_home)
    def _():
        here.start()

    @pl.when(jnp.logical_not(at_home))
    def _():
        away.start()

    for make, sem, n in sent:
        ref = make()
        pltpu.make_async_remote_copy(ref, ref, sem.at[n], sem.at[n], device_id=(r, c), device_id_type=MESH).wait_send()
    def all_sent(ref, sem):
        pltpu.make_async_remote_copy(ref, ref, sem, sem, device_id=(r, c), device_id_type=MESH).wait_send()

    all_sent(got, rsem)
    all_sent(parts.at[0:7], csem)
    all_sent(parts3.at[0:7], csem3)
    all_sent(gs_ref.at[0:15], gsem)
    all_sent(gt_ref.at[0:15], gsem3)

    @pl.when(at_home)
    def _():
        take(out.at[:, 0:1920], xrecv, (r, c))
        here.wait()
        all_sent(answer.at[0:15], xsem)

    @pl.when(jnp.logical_not(at_home))
    def _():
        take(out, xrecv, (r, c))
        all_sent(answer, xsem)


def invert(gs_ref, gt_ref, a_ref, x_ref, r_ref):
    gram = (gs_ref[...].reshape(256, 256) / 16384) * (gt_ref[...].reshape(256, 256) / 32768)
    eye = (lax.broadcasted_iota(jnp.int32, (256, 256), 0) == lax.broadcasted_iota(jnp.int32, (256, 256), 1)).astype(F32)
    diag = gram * eye
    down = 1 / jnp.sqrt(jnp.sum(diag, axis=1, keepdims=True))
    along = 1 / jnp.sqrt(jnp.sum(diag, axis=0, keepdims=True))
    a = gram * down * along
    a_ref[...] = a
    bound = jnp.max(jnp.sum(jnp.abs(a), axis=0, keepdims=True), axis=1, keepdims=True)
    scale = 2 / (1 + bound)
    x_ref[...] = eye * scale
    r_ref[...] = eye - a * scale

    def halves(w):
        hi = w.astype(BF)
        return hi, (w - hi.astype(F32)).astype(BF)

    def double(i, _):
        x, rest = x_ref[...], r_ref[...]
        xh, xl = halves(x)
        rh, rl = halves(rest)
        one = lax.dot_general(jnp.concatenate([rh, xh, rl, xl], 0), rh, NN, preferred_element_type=F32)
        two = lax.dot_general(jnp.concatenate([rh, xh], 0), rl, NN, preferred_element_type=F32)
        r_ref[...] = one[:256] + (one[512:768] + two[:256])
        x_ref[...] = x + (one[256:512] + (one[768:] + two[256:]))
        return 0

    lax.fori_loop(0, DOUBLINGS, double, 0)

    def dot(u, w):
        return lax.dot_general(u, w, NN, precision=HIGH, preferred_element_type=F32)

    def newton(i, _):
        now = x_ref[...]
        x_ref[...] = now + dot(now, eye - dot(a_ref[...], now))
        return 0

    lax.fori_loop(0, 3, newton, 0)
    a_ref[...] = x_ref[...] * down * along


DOUBLINGS = 20
EVENTS = (1, 3, 5, 7, 9, 11, 13, 15)
SECOND_AT = (1, 3, 10, 15)


def main(piece, spiece, third, values, length, live, sec, own):
    D = pltpu.SemaphoreType.DMA
    smem = pl.BlockSpec(memory_space=pltpu.SMEM)
    return pl.pallas_call(
        main_body,
        out_shape=(jax.ShapeDtypeStruct((16, 2048), F32), jax.ShapeDtypeStruct((2, 256, GRP, 128), BF)),
        in_specs=[ANY, ANY, INV, INV, smem, ANY, INV, INV],
        out_specs=(INV, ANY),
        scratch_shapes=[
            VMEM((4, 4, 2, 4, 16, 4096), BF), VMEM((2, 4, 2, 16, 2048), BF), VMEM((2, 16, 2048), BF), VMEM((2, 16, 2048), BF),
            VMEM((16, 256), F32), VMEM((8, 16, 256), F32),
            VMEM((2, UB * PAD, 128), F32), VMEM((2, UB * PAD, 128), F32),
            VMEM((256, GRP, 128), BF), VMEM((256, GRP, 128), BF), VMEM((512, 256), F32), VMEM((256, 512), F32), VMEM((512, 128), F32), pltpu.SMEM((1,), jnp.int32),
            VMEM((16, 16, 256), F32), VMEM((16, 16, 256), F32), VMEM((8, 256, 128), F32), VMEM((7, 256, 128), F32),
            VMEM((256, 256), F32), VMEM((256, 256), F32), VMEM((256, 256), F32), VMEM((16, 256), F32), VMEM((8, 16, 256), F32), VMEM((16, 16, 128), F32),
            D((SENDS,)), D((SEMS,)), D((14,)), D((14,)), *[D(())] * 4, D((16,)), D((3,)), D((4,)), *[D(())] * 8,
        ],
        compiler_params=pltpu.CompilerParams(has_side_effects=True, vmem_limit_bytes=67043328, collective_id=0),
        name="factor_update",
    )(piece, spiece, third, values, length, live, sec, own)


def per_device(values, length, owner, second, third, live_blocks, second_factor, third_factor):
    out, _ = main(third_factor.T, second_factor.T, third, values, length, live_blocks, second.reshape(1, 512), owner.reshape(1, 512))
    return out.T


def solution(mesh):
    both = P(("rows", "cols"))
    wide = P(("rows", "cols"), None)
    return jax.shard_map(
        per_device,
        mesh=mesh,
        in_specs=(wide, both, both, both, wide, both, P("cols", "rows"), P("cols", "rows")),
        out_specs=P("cols", "rows"),
        check_vma=False,
    )
```

```python
import jax
import jax.numpy as jnp
from jax import lax
from jax.experimental import pallas as pl
from jax.experimental.pallas import tpu as pltpu
from jax.sharding import PartitionSpec as P

F32 = jnp.float32
BF = jnp.bfloat16
MESH = pl.DeviceIdType.MESH
NT = (((1,), (1,)), ((), ()))
NN = (((1,), (0,)), ((), ()))
HIGH = lax.Precision.HIGHEST
VMEM = pltpu.VMEM
ANY = pl.BlockSpec(memory_space=pl.ANY)
INV = pl.BlockSpec(memory_space=pltpu.VMEM)

PARTS = ((0, 1152), (1152, 1408), (2560, 1536))
ORDERS = ("xyz", "yzx", "zxy")
SENDS = 12
SEMS = 75


def place():
    r, c = lax.axis_index("rows"), lax.axis_index("cols")
    return {"z": lax.div(r, 8) * 2 + lax.rem(c, 2), "x": lax.rem(lax.div(r, 2), 4), "k": lax.rem(r, 2), "y": lax.div(c, 2)}


def device(at):
    return (lax.div(at["z"], 2) * 8 + at["x"] * 2 + at["k"], at["y"] * 2 + lax.rem(at["z"], 2))


class Gather:
    def __init__(self, t, send, recv):
        self.t, self.send, self.recv = t, send, recv
        self.me = me = place()
        self.mine = device(me)
        self.steps = {d: [me[d], *(lax.rem(me[d] + i, 4) for i in (1, 2, 3))] for d in "zxy"}
        self.other = {**me, "k": 1 - me["k"]}
        self.used = 0

    def moved(self, at, dim, step):
        return {**at, dim: self.steps[dim][step]}

    def block(self, part, at, half=None):
        start, size = PARTS[part]
        if half is not None:
            first = (size // 128 // 2) * 128
            start, size = (start, first) if half == 0 else (start + first, size - first)
        return self.t.at[at["z"], at["x"], at["k"], at["y"], :, pl.ds(start, size)]

    def set_of(self, part, at, whole):
        start, size = PARTS[part]
        return self.t.at[*[slice(None) if d in whole else at[d] for d in "zxky"], :, pl.ds(start, size)]

    def new(self):
        self.used += 1
        return self.used - 1

    def copy(self, ref, n, to, group):
        c = pltpu.make_async_remote_copy(ref, ref, self.send.at[group], self.recv.at[n], device_id=device(to), device_id_type=MESH)
        c.start()

    def arrived(self, ref, n):
        pltpu.make_async_remote_copy(ref, ref, self.send.at[0], self.recv.at[n], device_id=self.mine, device_id_type=MESH).wait_recv()

    def run(self):
        me = self.me
        FORE, BACK = 1, 3
        parts = range(3)
        one = {(p, s): self.new() for p in parts for s in (FORE, BACK)}
        onef = {p: self.new() for p in parts}
        two = {(p, o, s): self.new() for p in parts for o in range(4) for s in (FORE, BACK)}
        twof = {p: self.new() for p in parts}
        three = {(p, b, s): self.new() for p in parts for b in range(4) for s in (FORE, BACK)}
        threef = {(p, o): self.new() for p in parts for o in range(4)}
        core = {p: self.new() for p in parts}

        def dims(p):
            return ORDERS[p]

        def at1(p, a):
            return self.moved(me, dims(p)[0], a)

        def at2(p, a, b):
            return self.moved(at1(p, a), dims(p)[1], b)

        def set3(p, b, c, k=None):
            d = dims(p)
            at = self.moved(self.moved(me, d[1], b), d[2], c)
            if k is not None:
                at = {**at, "k": k}
            return self.set_of(p, at, d[0])

        def to(p, i, s):
            return self.moved(me, dims(p)[i], s)

        def cross(p, b, c):
            self.copy(set3(p, b, c), core[p], self.other, p)

        def third(p, a, b):
            for s3 in (FORE, BACK):
                self.copy(self.block(p, at2(p, a, b)), three[p, b, s3], to(p, 2, s3), p)

        for p in parts:
            for s in (FORE, BACK):
                self.copy(self.block(p, me), one[p, s], to(p, 0, s), 6 + p)
        for p in parts:
            for s in (FORE, BACK):
                self.copy(self.block(p, me), two[p, 0, s], to(p, 1, s), 3 + p)
        for p in parts:
            third(p, 0, 0)
        yield
        for p in parts:
            for s in (FORE, BACK):
                back = 4 - s
                self.arrived(self.block(p, at1(p, back)), one[p, s])
                self.copy(self.block(p, at1(p, back), half=0 if s == FORE else 1), onef[p], to(p, 0, s), 9 + p)
                for s2 in (FORE, BACK):
                    self.copy(self.block(p, at1(p, back)), two[p, back, s2], to(p, 1, s2), 3 + p)
                third(p, back, 0)
        yield
        for p in parts:
            self.arrived(self.block(p, at1(p, 2)), onef[p])
            for s2 in (FORE, BACK):
                self.copy(self.block(p, at1(p, 2)), two[p, 2, s2], to(p, 1, s2), 3 + p)
            third(p, 2, 0)
            cross(p, 0, 0)
        yield
        FIRST = {FORE: (0, 3), BACK: (1, 2)}
        for o in (0, 3, 1, 2):
            for p in parts:
                for s in (FORE, BACK):
                    back = 4 - s
                    self.arrived(self.block(p, at2(p, o, back)), two[p, o, s])
                    if o in FIRST[s]:
                        self.copy(self.block(p, at2(p, o, back)), twof[p], to(p, 1, s), 6 + p)
                    third(p, o, back)
        for p in parts:
            for b in (3, 1):
                cross(p, b, 0)
        yield
        for p in parts:
            self.arrived(set3(p, 2, 0), twof[p])
            for o in (0, 3, 1, 2):
                third(p, o, 2)
            cross(p, 2, 0)
        for b in (0, 3, 1, 2):
            yield
            for p in parts:
                for s in (FORE, BACK):
                    back = 4 - s
                    self.arrived(set3(p, b, back), three[p, b, s])
                    if b in FIRST[s]:
                        self.copy(set3(p, b, back), threef[p, b], to(p, 2, s), 3 + p)
                    cross(p, b, back)
        yield
        for b in (0, 3, 1, 2):
            for p in parts:
                self.arrived(set3(p, b, 2), threef[p, b])
                cross(p, b, 2)
        for p in parts:
            start, size = PARTS[p]
            lanes = pl.ds(start, size)
            t = self.t
            self.arrived(t.at[:, :, self.other["k"], :, :, lanes], core[p])
            for n, ref in (
                (p, t.at[0:3, :, :, :, :, lanes]),
                (3 + p, t.at[0, 0:3, :, :, :, lanes]),
                (6 + p, t.at[0, 0, :, 0:3, :, lanes]),
                (9 + p, t.at[0, 0, 0, 0, :, lanes]),
            ):
                pltpu.make_async_remote_copy(ref, ref, self.send.at[n], self.recv.at[0], device_id=self.mine, device_id_type=MESH).wait_send()


UB = 16
STEPS = 512 // UB
GRP = 256
PAD = 129


def spread_pair(at, pair, ins, dst):
    third_ref, value_ref, length_ref, live_ref = ins
    lane = lax.broadcasted_iota(jnp.int32, (16, 128), 1)
    iq = lax.broadcasted_iota(jnp.int32, (128, 128), 0).astype(F32).astype(BF)
    ip = lax.broadcasted_iota(jnp.int32, (256, 128), 0).astype(F32).astype(BF)
    zero = jnp.zeros((128, 128), BF)

    def wide(one, n):
        return jnp.concatenate([one] * (n // 16), axis=0)

    qs, ps = [], []
    for j in range(2):
        b = at + 2 * pair + j
        third = jnp.broadcast_to(third_ref[pl.ds(b, 1), :], (16, 128))
        value = jnp.broadcast_to(value_ref[pl.ds(b, 1), :], (16, 128))
        used = jnp.where(b < live_ref[0], length_ref[b], 0)
        value = wide(jnp.where(lane < used, value, 0.0).astype(BF), 128)
        high = wide((third >> 8).astype(F32).astype(BF), 128)
        low = wide((third & 255).astype(F32).astype(BF), 256)
        qs.append(jnp.where(iq == high, value, zero))
        ps.append(jnp.where(ip == low, jnp.ones((), BF), jnp.zeros((), BF)))
    lhs = jnp.concatenate([jnp.concatenate([qs[0], zero], 1), jnp.concatenate([zero, qs[1]], 1)], 0)
    w = lax.dot_general(lhs, jnp.concatenate(ps, 1), NT, preferred_element_type=F32)
    for j in range(2):
        for h in range(2):
            dst[h, pl.ds((2 * pair + j) * PAD, 128), :] = w[j * 128:(j + 1) * 128, h * 128:(h + 1) * 128]


def split_rows(q, rows, src, whi, wlo):
    for h in range(2):
        f = src[h, pl.ds(q, UB, stride=PAD), :]
        hi = f.astype(BF)
        whi[q * 2 + h, rows, :] = hi
        wlo[q * 2 + h, rows, :] = (f - hi.astype(F32)).astype(BF)


def spread_split(at, rows, ins, src, dst, whi, wlo):
    for pair in range(UB // 2):
        spread_pair(at, pair, ins, dst)
        for q in range(pair * 16, pair * 16 + 16):
            split_rows(q, rows, src, whi, wlo)


def send_to(src, dst, ssem, rsem, to):
    c = pltpu.make_async_remote_copy(src, dst, ssem, rsem, device_id=to, device_id_type=MESH)
    c.start()
    return c


def take(ref, sem, me):
    pltpu.make_async_remote_copy(ref, ref, sem, sem, device_id=me, device_id_type=MESH).wait_recv()


def main_body(piece, spiece, third_ref, values_ref, length_ref, live_hbm, sec_ref, own_ref, out, spill,
              t, s_vm, near, far, part, parts, wfa, wfb, whi, wlo, fold, picked, value_ref, live_ref, gt_ref, gs_ref, total, got, a_ref, x_ref, r_ref, part3, parts3, answer,
              send, recv, ssem, srecv, csem, crecv, gsem, grecv, psem, lsem, lose, rsem, rrecv, xsem, xrecv, csem3, crecv3, gsem3, grecv3):
    r, c = lax.axis_index("rows"), lax.axis_index("cols")
    g = Gather(t, send, recv)
    me = g.me
    cp = pltpu.make_async_copy(piece, t.at[me["z"], me["x"], me["k"], me["y"]], lsem.at[0])
    cp.start()
    cs = pltpu.make_async_copy(spiece, s_vm.at[lax.div(me["z"], 2), me["x"], me["k"]], lsem.at[1])
    cs.start()
    home = lax.div(r, 2)
    at_home = home == c
    barrier = pltpu.get_barrier_semaphore()
    for to in [device(g.moved(me, d, way)) for d in "xyz" for way in (1, 3)] + [device(g.other)]:
        pl.semaphore_signal(barrier, inc=1, device_id=to, device_id_type=MESH)
    cl = pltpu.make_async_copy(live_hbm, live_ref, lsem.at[2])
    cl.start()
    cl.wait()
    value_ref[...] = values_ref[...].astype(F32)
    ins = (third_ref, value_ref, length_ref, live_ref)
    pl.semaphore_wait(barrier, 7)
    sent = []

    def push(src, dst, ssem, rsem, to):
        send_to(src, dst, ssem, rsem, to)

    cp.wait()
    run = g.run()
    next(run)
    cs.wait()
    FORE, BACK = 1, 3
    relay = {FORE: near, BACK: far}

    def hop(src, dst, n, to):
        send_to(src(), dst(), ssem.at[n], srecv.at[n], device(to))
        sent.append((src, ssem, n))

    xs = g.steps["x"]
    zs = [lax.div(z, 2) for z in g.steps["z"]]

    def plane(z, x=None, half=None):
        ref = s_vm.at[zs[z], slice(None) if x is None else xs[x], me["k"]]
        return ref if half is None else ref.at[:, pl.ds(half * 1024, 1024)]

    def stop(way, j):
        return relay[way].at[j]

    for n, way in enumerate((FORE, BACK)):
        hop(lambda: plane(0, 0), lambda: plane(0, 0), n, g.moved(me, "x", way))

    def second_one():
        for n, way in enumerate((FORE, BACK)):
            take(plane(0, 4 - way), srecv.at[n], (r, c))
            half = lambda n=n, way=way: plane(0, 4 - way, half=n)
            hop(half, half, 2 + n, g.moved(me, "x", way))

    def second_two():
        for n, way in enumerate((FORE, BACK)):
            take(plane(0, 2, half=n), srecv.at[2 + n], (r, c))
        for n, way in enumerate((FORE, BACK)):
            for j in range(2):
                hop(lambda n=n, j=j: plane(0, 2 * n + j), lambda: stop(way, j), 4 + 2 * n + j, g.moved(me, "z", way))
        hop(lambda: plane(0), lambda: plane(0), 12, g.other)

    def second_three():
        for n, way in enumerate((FORE, BACK)):
            for j in range(2):
                take(stop(way, j), srecv.at[4 + 2 * n + j], (r, c))
                hop(lambda way=way, j=j: stop(way, j), lambda: plane(4 - way, 2 * n + j), 8 + 2 * n + j, g.moved(me, "z", way))

    def second_four():
        for n in range(2):
            for j in range(2):
                take(plane(2, 2 * n + j), srecv.at[8 + 2 * n + j], (r, c))
        hop(lambda: plane(2), lambda: plane(2), 13, g.other)

    mine = gs_ref.at[r]

    mine3 = gt_ref.at[r]

    def third_gram():
        y, low = me["y"], lax.rem(me["z"], 2)
        whole = jnp.concatenate([t[low + 2 * h, :, :, y].reshape(128, 4096) for h in range(2)], 0)
        chunk = lax.dot_general(t[me["z"], me["x"], me["k"], y], whole, NT, preferred_element_type=F32)
        part3[...] = chunk
        parts3[c] = chunk
        for i in range(1, 8):
            push(part3, parts3.at[c], csem3, crecv3, (r, lax.rem(c + i, 8)))

    def third_gram_sum():
        take(parts3.at[0:7], crecv3, (r, c))
        gt_ref[r] = sum(parts3[i] for i in range(8))
        for i in range(1, 16):
            push(mine3, mine3, gsem3, grecv3, (lax.rem(r + i, 16), c))

    def second_gram():
        for n, z in ((12, 0), (13, 2)):
            take(s_vm.at[zs[z], :, g.other["k"]], srecv.at[n], (r, c))
        chunk = lax.dot_general(s_vm[zs[0], me["x"], me["k"]], s_vm[...].reshape(256, 2048), NT, preferred_element_type=F32)
        part[...] = chunk
        parts[c] = chunk
        for i in range(1, 8):
            push(part, parts.at[c], csem, crecv, (r, lax.rem(c + i, 8)))

    def second_gram_sum():
        take(parts.at[0:7], crecv, (r, c))
        gs_ref[r] = sum(parts[i] for i in range(8))
        for i in range(1, 16):
            push(mine, mine, gsem, grecv, (lax.rem(r + i, 16), c))

    def parked(step):
        both = spill.at[:, :, pl.ds(pl.multiple_of(step * UB, UB), UB), :]
        pltpu.make_async_copy(both, both, psem.at[step]).wait()

    def park(step):
        rows = pl.ds(pl.multiple_of(step * UB, UB), UB)
        return (
            pltpu.make_async_copy(whi.at[:, rows, :], spill.at[0, :, rows, :], psem.at[step]),
            pltpu.make_async_copy(wlo.at[:, rows, :], spill.at[1, :, rows, :], psem.at[step]),
        )

    todo = {j: [] for j in range(STEPS // 2)}
    for j in EVENTS:
        todo[j].append(lambda: next(run))
    for j, f in zip(SECOND_AT, (second_one, second_two, second_three, second_four)):
        todo[j].append(f)

    def iteration(i, _):
        for j in range(STEPS // 2):
            if todo[j]:
                @pl.when(i == j)
                def _():
                    for f in todo[j]:
                        f()
        for half in range(2):
            step = lax.rem(2 * i + half + STEPS - 1, STEPS)
            slot = lax.rem(step, 16)

            @pl.when((step >= 16) & (2 * i + half >= 1))
            def _():
                parked(slot)

            rows = pl.ds(pl.multiple_of(slot * UB, UB), UB)
            at = pl.multiple_of((2 * i + half) * UB, UB)
            src, dst = ((wfb, wfa), (wfa, wfb))[half]
            spread_split(at, rows, ins, src, dst, whi, wlo)

            @pl.when(step < 16)
            def _():
                for x in park(slot):
                    x.start()
        return 0

    lax.fori_loop(0, STEPS // 2, iteration, 0)
    parked(15)
    for q in range(128):
        split_rows(q, pl.ds(GRP - UB, UB), wfb, whi, wlo)
    second_gram()
    one, zero = jnp.ones((), BF), jnp.zeros((), BF)
    second = jnp.zeros((256, 512), F32)
    for j in range(4):
        ij = lax.broadcasted_iota(jnp.int32, (512, 512), 0) + j * 512
        pick = jnp.where(ij == sec_ref[...] - c * 2048, one, zero)
        second += lax.dot_general(s_vm[:, :, :, :, j * 512:(j + 1) * 512].reshape(256, 512), pick, NN, preferred_element_type=F32)
    picked[...] = second
    for _ in run:
        pass

    def back(i):
        tiles = pl.ds(pl.multiple_of(i * 64, 64), 64)
        return (
            pltpu.make_async_copy(spill.at[0, tiles], whi.at[tiles], lose.at[i]),
            pltpu.make_async_copy(spill.at[1, tiles], wlo.at[tiles], lose.at[i]),
        )

    third_gram()
    fold[...] = jnp.zeros((512, 256), F32)
    for first in (True, False):
        def dense(i, _):
            if not first:
                both = spill.at[:, pl.ds(pl.multiple_of(i * 64, 64), 64)]
                pltpu.make_async_copy(both, both, lose.at[i]).wait()
            tt = jnp.concatenate(
                [jnp.concatenate([t[low + 2 * h, :, :, i].reshape(128, 4096) for h in range(2)], 0) for low in range(2)], 1
            )
            side = lambda w: jnp.concatenate([w[i * 64 + j] for j in range(64)], 1)
            lhs = jnp.concatenate([side(whi), side(wlo)], 0)
            res = lax.dot_general(lhs, tt, NT, preferred_element_type=F32)
            fold[pl.ds(GRP if first else 0, GRP), :] += res[:GRP] + res[GRP:]
            if first:
                for x in back(i):
                    x.start()
            return 0

        lax.fori_loop(0, 4, dense, 0)
        if first:
            second_gram_sum()
            third_gram_sum()

    contrib = picked[...] * fold[...].T
    hi = contrib.astype(BF)
    lhs = jnp.concatenate([hi, (contrib - hi.astype(F32)).astype(BF)], 0)
    for turn in range(4):
        j = lax.rem(lax.div(c, 2) + 1 + turn, 4)
        ii = lax.broadcasted_iota(jnp.int32, (256, 512), 0) + j * 256
        put = jnp.where(ii == own_ref[...] - r * 1024, one, zero)
        res = lax.dot_general(lhs, put, NT, preferred_element_type=F32)
        both = res[:256] + res[256:]
        for h in range(2):
            total[2 * j + h] = both[:, h * 128:(h + 1) * 128]
        for h in range(2):
            to = 2 * j + h

            @pl.when(c != to)
            def _():
                send_to(total.at[to], got.at[lax.rem(to - c + 8, 8) - 1], rsem, rrecv, (r, to))

    take(gs_ref.at[0:15], grecv, (r, c))
    take(gt_ref.at[0:15], grecv3, (r, c))
    invert(gs_ref, gt_ref, a_ref, x_ref, r_ref)
    rows = total[c]
    take(got, rrecv, (r, c))
    for i in range(7):
        rows = rows + got[i]
    answer[...] = lax.dot_general(a_ref[...], rows, NN, precision=HIGH, preferred_element_type=F32).reshape(16, 16, 128)

    slot = lax.rem(r, 2) * 8 + c
    lanes = pl.ds(pl.multiple_of(slot * 128, 128), 128)
    for i in range(1, 16):
        to = lax.rem(r + i, 16)
        send_to(answer.at[to], out.at[:, lanes], xsem, xrecv, (to, home))
    here = pltpu.make_async_copy(answer.at[r], out.at[:, lanes], lsem.at[0])
    away = pltpu.make_async_remote_copy(answer.at[r], out.at[:, lanes], xsem, xrecv, device_id=(r, home), device_id_type=MESH)

    @pl.when(at_home)
    def _():
        here.start()

    @pl.when(jnp.logical_not(at_home))
    def _():
        away.start()

    for make, sem, n in sent:
        ref = make()
        pltpu.make_async_remote_copy(ref, ref, sem.at[n], sem.at[n], device_id=(r, c), device_id_type=MESH).wait_send()
    def all_sent(ref, sem):
        pltpu.make_async_remote_copy(ref, ref, sem, sem, device_id=(r, c), device_id_type=MESH).wait_send()

    all_sent(got, rsem)
    all_sent(parts.at[0:7], csem)
    all_sent(parts3.at[0:7], csem3)
    all_sent(gs_ref.at[0:15], gsem)
    all_sent(gt_ref.at[0:15], gsem3)

    @pl.when(at_home)
    def _():
        take(out.at[:, 0:1920], xrecv, (r, c))
        here.wait()
        all_sent(answer.at[0:15], xsem)

    @pl.when(jnp.logical_not(at_home))
    def _():
        take(out, xrecv, (r, c))
        all_sent(answer, xsem)


def invert(gs_ref, gt_ref, a_ref, x_ref, r_ref):
    gram = (gs_ref[...].reshape(256, 256) / 16384) * (gt_ref[...].reshape(256, 256) / 32768)
    eye = (lax.broadcasted_iota(jnp.int32, (256, 256), 0) == lax.broadcasted_iota(jnp.int32, (256, 256), 1)).astype(F32)
    diag = gram * eye
    down = 1 / jnp.sqrt(jnp.sum(diag, axis=1, keepdims=True))
    along = 1 / jnp.sqrt(jnp.sum(diag, axis=0, keepdims=True))
    a = gram * down * along
    a_ref[...] = a
    bound = jnp.max(jnp.sum(jnp.abs(a), axis=0, keepdims=True), axis=1, keepdims=True)
    scale = 2 / (1 + bound)
    x_ref[...] = eye * scale
    r_ref[...] = eye - a * scale

    def halves(w):
        hi = w.astype(BF)
        return hi, (w - hi.astype(F32)).astype(BF)

    def double(i, _):
        x, rest = x_ref[...], r_ref[...]
        xh, xl = halves(x)
        rh, rl = halves(rest)
        one = lax.dot_general(jnp.concatenate([rh, xh, rl, xl], 0), rh, NN, preferred_element_type=F32)
        two = lax.dot_general(jnp.concatenate([rh, xh], 0), rl, NN, preferred_element_type=F32)
        r_ref[...] = one[:256] + (one[512:768] + two[:256])
        x_ref[...] = x + (one[256:512] + (one[768:] + two[256:]))
        return 0

    lax.fori_loop(0, DOUBLINGS, double, 0)

    def dot(u, w):
        return lax.dot_general(u, w, NN, precision=HIGH, preferred_element_type=F32)

    def newton(i, _):
        now = x_ref[...]
        x_ref[...] = now + dot(now, eye - dot(a_ref[...], now))
        return 0

    lax.fori_loop(0, 3, newton, 0)
    a_ref[...] = x_ref[...] * down * along


DOUBLINGS = 20
EVENTS = (1, 3, 5, 7, 9, 11, 13, 15)
SECOND_AT = (1, 3, 10, 15)


def main(piece, spiece, third, values, length, live, sec, own):
    D = pltpu.SemaphoreType.DMA
    smem = pl.BlockSpec(memory_space=pltpu.SMEM)
    return pl.pallas_call(
        main_body,
        out_shape=(jax.ShapeDtypeStruct((16, 2048), F32), jax.ShapeDtypeStruct((2, 256, GRP, 128), BF)),
        in_specs=[ANY, ANY, INV, INV, smem, ANY, INV, INV],
        out_specs=(INV, ANY),
        scratch_shapes=[
            VMEM((4, 4, 2, 4, 16, 4096), BF), VMEM((2, 4, 2, 16, 2048), BF), VMEM((2, 16, 2048), BF), VMEM((2, 16, 2048), BF),
            VMEM((16, 256), F32), VMEM((8, 16, 256), F32),
            VMEM((2, UB * PAD, 128), F32), VMEM((2, UB * PAD, 128), F32),
            VMEM((256, GRP, 128), BF), VMEM((256, GRP, 128), BF), VMEM((512, 256), F32), VMEM((256, 512), F32), VMEM((512, 128), F32), pltpu.SMEM((1,), jnp.int32),
            VMEM((16, 16, 256), F32), VMEM((16, 16, 256), F32), VMEM((8, 256, 128), F32), VMEM((7, 256, 128), F32),
            VMEM((256, 256), F32), VMEM((256, 256), F32), VMEM((256, 256), F32), VMEM((16, 256), F32), VMEM((8, 16, 256), F32), VMEM((16, 16, 128), F32),
            D((SENDS,)), D((SEMS,)), D((14,)), D((14,)), *[D(())] * 4, D((16,)), D((3,)), D((4,)), *[D(())] * 8,
        ],
        compiler_params=pltpu.CompilerParams(has_side_effects=True, vmem_limit_bytes=67043328, collective_id=0),
        name="factor_update",
    )(piece, spiece, third, values, length, live, sec, own)


def per_device(values, length, owner, second, third, live_blocks, second_factor, third_factor):
    out, _ = main(third_factor.T, second_factor.T, third, values, length, live_blocks, second.reshape(1, 512), owner.reshape(1, 512))
    return out.T


def solution(mesh):
    both = P(("rows", "cols"))
    wide = P(("rows", "cols"), None)
    return jax.shard_map(
        per_device,
        mesh=mesh,
        in_specs=(wide, both, both, both, wide, both, P("cols", "rows"), P("cols", "rows")),
        out_specs=P("cols", "rows"),
        check_vma=False,
    )
```
